256 devices in a mesh: tm: 32 (over y, z), tensor: 8 (over x, core).
Axes of the slice: x: 4, y: 4, z: 8, core: 2. Of those that a mesh axis runs over, the one named last changes fastest.
Arguments:
- frames_in: bfloat16 [32, 520, 1024], P('tm'), may hold values from -6 to 6
- frame_time: int32 [16], replicated, may hold values from 0 to 15, each once
- cond_count: int32 [16], replicated, may hold values from 0 to 2
- ln1_gain: float32 [2, 1024], replicated, may hold values from 0.5 to 1.5
- ln1_bias: float32 [2, 1024], replicated, may hold values from -1.75 to 1.75
- qkv_weight: bfloat16 [2, 3, 1024, 1024], P(None, None, None, 'tensor'), may hold values from -17 to 17
- qkv_bias: float32 [2, 3, 1024], P(None, None, 'tensor'), may hold values from -1.75 to 1.75
- out_weight: bfloat16 [2, 1024, 1024], P(None, 'tensor'), may hold values from -0.1875 to 0.1875
- out_bias: float32 [2, 1024], replicated, may hold values from -1.75 to 1.75
- ln2_gain: float32 [2, 1024], replicated, may hold values from 0.5 to 1.5
- ln2_bias: float32 [2, 1024], replicated, may hold values from -1.75 to 1.75
- fc1_weight: bfloat16 [2, 1024, 4096], P(None, None, 'tensor'), may hold values from -0.1875 to 0.1875
- fc1_bias: float32 [2, 4096], P(None, 'tensor'), may hold values from -3 to 3
- fc2_weight: bfloat16 [2, 4096, 1024], P(None, 'tensor'), may hold values from -0.09375 to 0.09375
- fc2_bias: float32 [2, 1024], replicated, may hold values from -1.75 to 1.75
Outputs:
- frames_out: bfloat16 [32, 520, 1024], P('tm', 'tensor')
The draws below stay inside these ranges and needn't reach their ends.
Inputs may be any that keep to these rules, and one draw needn't show every extreme that they name: `frame_time`: every time index 0 to 15 appears once. `cond_count`: the valid action and state tokens of a frame are its first ones.
All inputs are finite; a program needn't handle non-finite values.
Results may differ from the reference program's by a relative error of at most 0.04.
Values may be sent and summed in bfloat16 or wider, within the bound.
No kernel may reach another device: no remote copies, remote signals or barrier semaphores. Data moves between devices by JAX's collectives and lax.ppermute only.
A program may use at most 128 MiB of HBM per device.

```python
import jax
import jax.numpy as jnp
from jax import lax

D = 1024
HEADS = 16
FF = 4096
PATCH_DEV = 64
COND = 2
SEQS = 8
LAYERS = 2
FRAMES = 16
ROWS = 520
N_TM = 32


def draw_qkv_weight(key, part):
    weights_raw = jnp.clip(jax.random.normal(jax.random.fold_in(key, 101), (LAYERS, 3, D, D), jnp.float32), -5.0, 5.0) * D ** (-0.5)
    return weights_raw.astype(jnp.bfloat16)


def plant(values, stream_key, low, high):
    longest = values.shape.index(max(values.shape))
    spots = []
    for shift in (0, 1):
        where = [jax.random.randint(jax.random.fold_in(stream_key, axis), (), 0, length) for axis, length in enumerate(values.shape)]
        where[longest] = (where[longest] + shift) % values.shape[longest]
        spots.append(tuple(where))
    return values.at[spots[0]].set(low).at[spots[1]].set(high)


def shard_levels(rng, shape, cuts, low, largest):
    gain, own = 1.0, jax.random.fold_in(rng, 6)
    for dim, parts in cuts:
        draws = jnp.exp(jax.random.uniform(jax.random.fold_in(own, dim), (parts,), jnp.float32, low / len(cuts), largest / len(cuts)))
        gain = gain * jnp.repeat(draws, shape[dim] // parts).reshape([-1 if axis == dim else 1 for axis in range(len(shape))])
    return gain


def normal_values(rng, dims, scale, limit, split=(), kind=jnp.bfloat16):
    array = jax.random.normal(rng, dims, jnp.float32) * scale
    if len(split) > 0:
        array = shard_levels(rng, dims, split, -0.22, 0.18) * array
    return jnp.clip(array, min=-limit, max=limit).astype(kind)


def setup_inputs(seed: int = 0) -> dict:
    keys = jax.random.split(jax.random.key(seed), 16)
    return {
        "frames_in": normal_values(keys[0], (N_TM, ROWS, D), 1.0, 6.0, ((0, 32),)),
        "frame_time": jax.random.permutation(keys[1], FRAMES).astype(jnp.int32),
        "cond_count": plant(jax.random.randint(keys[2], (FRAMES,), 0, COND + 1), jax.random.fold_in(keys[2], 1), 0, COND).astype(jnp.int32),
        "ln1_gain": jnp.clip(1.0 + 0.1 * jax.random.normal(keys[3], (LAYERS, D), jnp.float32), 0.5, 1.5),
        "ln1_bias": normal_values(keys[4], (LAYERS, D), 0.3, 1.75, (), jnp.float32),
        "qkv_weight": draw_qkv_weight(jax.random.fold_in(keys[15], 71), 0),
        "qkv_bias": normal_values(keys[6], (LAYERS, 3, D), 0.3, 1.75, ((2, 8),), jnp.float32),
        "out_weight": normal_values(keys[7], (LAYERS, D, D), D ** -0.5, 0.1875, ((1, 8),)),
        "out_bias": normal_values(keys[8], (LAYERS, D), 0.3, 1.75, (), jnp.float32),
        "ln2_gain": jnp.clip(1.0 + 0.1 * jax.random.normal(keys[9], (LAYERS, D), jnp.float32), 0.5, 1.5),
        "ln2_bias": normal_values(keys[10], (LAYERS, D), 0.3, 1.75, (), jnp.float32),
        "fc1_weight": normal_values(keys[11], (LAYERS, D, FF), D ** -0.5, 0.1875, ((2, 8),)),
        "fc1_bias": normal_values(keys[12], (LAYERS, FF), 0.5, 3.0, ((1, 8),), jnp.float32),
        "fc2_weight": normal_values(keys[13], (LAYERS, FF, D), FF ** -0.5, 0.09375, ((1, 8),)),
        "fc2_bias": normal_values(keys[14], (LAYERS, D), 0.3, 1.75, (), jnp.float32),
    }


def layer_norm(inputs, gain_row, bias_row):
    center = lax.optimization_barrier(jnp.mean(inputs, axis=-1, keepdims=True))
    spread = lax.optimization_barrier(jnp.mean(jnp.square(inputs - center), axis=-1, keepdims=True))
    return (inputs - center) * lax.rsqrt(spread + 1e-06) * gain_row + bias_row

def piece_tables(frame_time, cond_count, piece_count, frame_split, piece_rows):
    cond_dev = COND // frame_split
    piece_ids = jnp.arange(piece_count, dtype=jnp.int32)
    frame_ids = jnp.arange(frame_time.shape[0], dtype=jnp.int32)
    matches = (piece_ids // frame_split)[:, None] == frame_ids[None, :]
    piece_time = lax.optimization_barrier(jnp.sum(jnp.where(matches, frame_time[None, :], 0), axis=1)).astype(jnp.int32)
    piece_cond = lax.optimization_barrier(jnp.sum(jnp.where(matches, cond_count[None, :], 0), axis=1)).astype(jnp.int32)
    slot_index = jnp.arange(piece_rows, dtype=jnp.int32)
    cond_slot = (piece_ids % frame_split)[:, None] * cond_dev + slot_index[None, :] - PATCH_DEV
    valid = (slot_index[None, :] < PATCH_DEV) | (cond_slot < piece_cond[:, None])
    return (piece_time, valid)

def reference(frames_in, frame_time, cond_count, ln1_gain, ln1_bias, qkv_weight, qkv_bias, out_weight, out_bias, ln2_gain, ln2_bias, fc1_weight, fc1_bias, fc2_weight, fc2_bias):
    frame_split = N_TM // FRAMES
    cond_dev = COND // frame_split
    piece_rows = PATCH_DEV + cond_dev
    piece_time, valid = piece_tables(frame_time, cond_count, N_TM, frame_split, piece_rows)
    head_dim = D // HEADS
    scale = head_dim ** (-0.5)
    stream = frames_in
    for layer_idx in range(LAYERS):
        flattened = stream.reshape(-1, D).astype(jnp.float32)
        normed = layer_norm(flattened, ln1_gain[layer_idx], ln1_bias[layer_idx]).astype(jnp.bfloat16)
        projected = []
        for part_idx in range(3):
            result = jnp.dot(normed, qkv_weight[layer_idx, part_idx], preferred_element_type=jnp.float32) + qkv_bias[layer_idx, part_idx]
            result = lax.optimization_barrier(result.astype(jnp.bfloat16))
            projected.append(result.astype(jnp.float32).reshape(N_TM, SEQS, piece_rows, HEADS, head_dim))
        queries, keys_all, values_all = projected

        def one_piece(piece_idx):
            query_block = lax.dynamic_index_in_dim(queries, piece_idx, 0, keepdims=False)
            scores = jnp.einsum('sqhd,gskhd->shqgk', query_block, keys_all) * scale
            my_time = lax.dynamic_index_in_dim(piece_time, piece_idx, 0, keepdims=False)
            allowed = (piece_time <= my_time)[:, None] & valid
            scores = jnp.where(allowed, scores, -1e+30)
            highest = lax.optimization_barrier(jnp.max(scores, axis=(3, 4), keepdims=True))
            weights = jnp.where(allowed, jnp.exp(scores - highest), 0.0)
            totals = lax.optimization_barrier(jnp.sum(weights, axis=(3, 4)))
            rounded = lax.optimization_barrier(weights.astype(jnp.bfloat16)).astype(jnp.float32)
            mixed = jnp.einsum('shqgk,gskhd->shqd', rounded, values_all) / totals[..., None]
            return jnp.transpose(mixed, (0, 2, 1, 3)).reshape(SEQS * piece_rows, D).astype(jnp.bfloat16)
        attended = lax.map(one_piece, jnp.arange(N_TM, dtype=jnp.int32))
        projection = jnp.dot(attended.reshape(-1, D), out_weight[layer_idx], preferred_element_type=jnp.float32)
        first = flattened + projection + out_bias[layer_idx]
        normed_two = layer_norm(first, ln2_gain[layer_idx], ln2_bias[layer_idx]).astype(jnp.bfloat16)
        inner = jax.nn.gelu(jnp.dot(normed_two, fc1_weight[layer_idx], preferred_element_type=jnp.float32) + fc1_bias[layer_idx], approximate=False).astype(jnp.bfloat16)
        output = jnp.dot(inner, fc2_weight[layer_idx], preferred_element_type=jnp.float32)
        stream = (first + output + fc2_bias[layer_idx]).astype(jnp.bfloat16).reshape(N_TM, SEQS * piece_rows, D)
    return stream
```

```python
import functools

import jax
import jax.numpy as jnp
from jax import lax
from jax.experimental import pallas as pl
from jax.experimental.pallas import tpu as pltpu
from jax.sharding import PartitionSpec as P

D = 1024
LAYERS = 2
CLIPS = 8
PARTS = 32
SLOTS = 65
BLOCK = 65
PAD = 72
KEYS = 2176
NX = 4
LOG2E = 1.4426950408889634
SCALE = 0.125 * LOG2E
NEG = -1e30


def lanes(shape):
    return lax.broadcasted_iota(jnp.int32, shape, len(shape) - 1)


def norm(rows, gain, bias):
    center = jnp.mean(rows, axis=-1, keepdims=True)
    off = rows - center
    spread = jnp.mean(off * off, axis=-1, keepdims=True)
    return off * lax.rsqrt(spread + 1e-06) * gain + bias


def prep_kernel(idx, x_ref, g_ref, b_ref, n0, n1, n2, n3, own):
    x, k = idx[0], idx[1]
    gain, bias = g_ref[0:1, :], b_ref[0:1, :]
    half = pl.ds(pl.multiple_of(k * 32, 32), 32)
    for s, out in enumerate((n0, n1, n2, n3)):
        chip = lax.rem(x + s, NX)
        for b in range(2):
            rows = x_ref[2 * chip + b, half, :]
            out[32 * b : 32 * b + 32, :] = norm(rows.astype(jnp.float32), gain, bias).astype(jnp.bfloat16)
            if s == 0:
                own[32 * b : 32 * b + 32, :] = rows
        rows = x_ref[2 * chip + k, 64:65, :]
        out[64:65, :] = norm(rows.astype(jnp.float32), gain, bias).astype(jnp.bfloat16)
        if s == 0:
            own[64:65, :] = rows


def qkv_kernel(idx, n0, n1, n2, n3, w_own, w_par, b_own, b_par, out, rows):
    k = idx[1]
    for s, n in enumerate((n0, n1, n2, n3)):
        rows[72 * s : 72 * s + 65, :] = n[...]
    low = lanes((NX * PAD, 128)) < 64
    low8 = lanes((8, 128)) < 64
    sub = lax.broadcasted_iota(jnp.int32, (8, 128), 0)
    for w, bias, side in ((w_own, b_own, k), (w_par, b_par, 1 - k)):
        q, key, val = (
            jnp.dot(rows[...], w[0, i], preferred_element_type=jnp.float32) + bias[0, i : i + 1, :]
            for i in range(3)
        )
        q_r, key_r, val_r = (pltpu.roll(a, 64, 1) for a in (q, key, val))
        for hl in range(2):
            head = 2 * side + hl
            if hl == 0:
                kv = jnp.where(low, key, val_r)
                q_lo, q_hi = q, q_r
            else:
                kv = jnp.where(low, key_r, val)
                q_lo, q_hi = q_r, q
            for s in range(NX):
                for b in range(2):
                    at = 72 * s + 32 * b
                    slot = s * 8 + b * 4 + head
                    out[slot, 0:32, :] = kv[at : at + 32].astype(jnp.bfloat16)
                    out[slot, 32:48, :] = jnp.where(
                        low[:16], q_lo[at : at + 16], q_hi[at + 16 : at + 32]
                    ).astype(jnp.bfloat16)
                    out[slot, 48:56, :] = jnp.zeros((8, 128), jnp.bfloat16)
            for s in range(NX):
                at = 72 * s + 64
                tail = jnp.where(
                    sub == 0,
                    jnp.broadcast_to(kv[at : at + 1], (8, 128)),
                    jnp.where((sub == 1) & low8, jnp.broadcast_to(q_lo[at : at + 1], (8, 128)), 0.0),
                )
                out[s * 8 + k * 4 + head, 48:56, :] = tail.astype(jnp.bfloat16)


def attn_kernel(idx, times, r_own, r_par, key_time, part_time, out, kv, score, prob, total):
    core, mine = idx[1], idx[2]
    kv[0:1024, :] = r_own[:, 0:32, :].reshape(1024, 128)
    kv[1024:2048, :] = r_par[:, 0:32, :].reshape(1024, 128)
    sub = lax.broadcasted_iota(jnp.int32, (PARTS, 8, 128), 1)
    tail_own = r_own[:, 48:56, :].astype(jnp.float32)
    tail_par = r_par[:, 48:56, :].astype(jnp.float32)
    extra = jnp.sum(jnp.where(sub == 0, jnp.where(mine == 1, tail_own, tail_par), 0.0), axis=1)
    kv[2048:2080, :] = extra.astype(jnp.bfloat16)
    kv[2080:KEYS, :] = jnp.zeros((KEYS - 2080, 128), jnp.bfloat16)
    q_extra = jnp.sum(jnp.where(sub == 1, tail_own, 0.0), axis=1).astype(jnp.bfloat16)
    low = lanes((128, 128)) < 64
    contract_last = (((1,), (1,)), ((), ()))

    def tile(t, carry):
        packed = r_own[pl.ds(t * 8, 8), 32:48, :].reshape(128, 128).astype(jnp.float32)
        q = jnp.concatenate(
            [jnp.where(low, packed, 0.0), jnp.where(low, pltpu.roll(packed, 64, 1), 0.0)], axis=0
        ).astype(jnp.bfloat16)
        score[...] = lax.dot_general(q, kv[...], contract_last, preferred_element_type=jnp.float32)
        for part in range(8):
            seen = key_time[...] <= times[t * 8 + part]
            for side in range(2):
                at = side * 128 + part * 16
                now = jnp.where(seen, score[at : at + 16, :] * SCALE, NEG)
                weights = jnp.exp2(now - jnp.max(now, axis=1, keepdims=True))
                prob[at : at + 16, :] = weights.astype(jnp.bfloat16)
                total[at : at + 16, :] = jnp.broadcast_to(
                    jnp.sum(weights, axis=1, keepdims=True), (16, 128)
                )
        mixed = jnp.dot(prob[...], kv[...], preferred_element_type=jnp.float32) / total[...]
        merged = jnp.where(low, pltpu.roll(mixed[:128], 64, 1), mixed[128:])
        out[pl.ds(t * 8, 8), 0:16, :] = merged.astype(jnp.bfloat16).reshape(8, 16, 128)
        return carry

    lax.fori_loop(0, 4, tile, 0)
    now = lax.dot_general(q_extra, kv[...], contract_last, preferred_element_type=jnp.float32)
    now = jnp.where(key_time[...] <= part_time[:, 0:1], now * SCALE, NEG)
    weights = jnp.exp2(now - jnp.max(now, axis=1, keepdims=True))
    mixed = jnp.dot(weights.astype(jnp.bfloat16), kv[...], preferred_element_type=jnp.float32)
    mixed = mixed / jnp.sum(weights, axis=1, keepdims=True)
    mixed = pltpu.roll(mixed, 64, 1)
    out[:, 16:24, :] = jnp.broadcast_to(mixed[:, None, :], (PARTS, 8, 128)).astype(jnp.bfloat16)


def out_kernel(idx, back, w_own, w_par, p0, p1, p2, p3, left, right):
    k = idx[1]
    low = lanes((24, 128)) < 64

    def pair(first, second):
        first, second = first.astype(jnp.float32), second.astype(jnp.float32)
        return (
            jnp.where(low, first, pltpu.roll(second, 64, 1)),
            jnp.where(low, pltpu.roll(first, 64, 1), second),
        )

    for s in range(NX):
        for dst, h in ((left, 0), (right, 2)):
            for b in range(2):
                slot = s * 8 + b * 4 + h
                lo, hi = pair(back[slot], back[slot + 1])
                at = 72 * s + 32 * b
                dst[at : at + 16, :] = lo[:16].astype(jnp.bfloat16)
                dst[at + 16 : at + 32, :] = hi[:16].astype(jnp.bfloat16)
            slot = s * 8 + k * 4 + h
            lo, _ = pair(back[slot], back[slot + 1])
            dst[72 * s + 64 : 72 * s + 72, :] = lo[16:24].astype(jnp.bfloat16)
    first = jnp.where(k == 0, left[...], right[...])
    second = jnp.where(k == 0, right[...], left[...])
    for j in range(4):
        cols = slice(256 * j, 256 * j + 256)
        partial = jnp.dot(first, w_own[0, :, cols], preferred_element_type=jnp.float32) + jnp.dot(
            second, w_par[0, :, cols], preferred_element_type=jnp.float32
        )
        for s, out in enumerate((p0, p1, p2, p3)):
            out[:, cols] = partial[72 * s : 72 * s + 65].astype(jnp.bfloat16)


def mid_kernel(layer, own, p0, p1, p2, p3, o_bias, gain, bias, first, normed):
    rows = own[...].astype(jnp.float32)
    summed = (p0[...].astype(jnp.float32) + p1[...].astype(jnp.float32)) + (
        p2[...].astype(jnp.float32) + p3[...].astype(jnp.float32)
    )
    rows = rows + summed + o_bias[layer : layer + 1, :]
    first[...] = rows
    normed[...] = norm(rows, gain[layer : layer + 1, :], bias[layer : layer + 1, :]).astype(jnp.bfloat16)


def mlp_kernel(n0, n1, n2, n3, w1_own, w1_par, b1_own, b1_par, w2_own, w2_par, y0, y1, y2, y3, rows):
    for s, n in enumerate((n0, n1, n2, n3)):
        rows[72 * s : 72 * s + 65, :] = n[...]
    total = jnp.zeros((NX * PAD, D), jnp.float32)
    for w1, b1, w2 in ((w1_own, b1_own, w2_own), (w1_par, b1_par, w2_par)):
        inner = jnp.dot(rows[...], w1[0], preferred_element_type=jnp.float32) + b1[...]
        inner = (0.5 * inner * (1.0 + lax.erf(inner * 0.7071067811865476))).astype(jnp.bfloat16)
        total = total + jnp.dot(inner, w2[0], preferred_element_type=jnp.float32)
    for s, out in enumerate((y0, y1, y2, y3)):
        out[...] = total[72 * s : 72 * s + 65].astype(jnp.bfloat16)


def end_kernel(layer, first, y0, y1, y2, y3, o_bias, gain, bias, stream, normed):
    summed = (y0[...].astype(jnp.float32) + y1[...].astype(jnp.float32)) + (
        y2[...].astype(jnp.float32) + y3[...].astype(jnp.float32)
    )
    rows = (first[...] + summed + o_bias[layer : layer + 1, :]).astype(jnp.bfloat16)
    stream[...] = rows
    normed[...] = norm(
        rows.astype(jnp.float32), gain[layer + 1 : layer + 2, :], bias[layer + 1 : layer + 2, :]
    ).astype(jnp.bfloat16)


def last_kernel(layer, idx, first, y0, y1, y2, y3, o_bias, stream, send):
    k = idx[1]
    summed = (y0[...].astype(jnp.float32) + y1[...].astype(jnp.float32)) + (
        y2[...].astype(jnp.float32) + y3[...].astype(jnp.float32)
    )
    rows = (first[...] + summed + o_bias[layer : layer + 1, :]).astype(jnp.bfloat16)
    stream[...] = rows
    send[...] = jnp.where(k == 0, rows[32:64], rows[0:32])


def place_kernel(idx, stream, recv, out):
    k = idx[1]
    out[0, 0:32, :] = jnp.where(k == 0, stream[0:32, :], recv[...])
    out[0, 32:64, :] = jnp.where(k == 0, recv[...], stream[32:64, :])
    out[0, 64:65, :] = stream[64:65, :]


VMEM = pl.BlockSpec(memory_space=pltpu.VMEM)
SMEM = pl.BlockSpec(memory_space=pltpu.SMEM)


def of_layer(layer, array):
    rest = array.shape[1:]
    zeros = (0,) * len(rest)
    return pl.BlockSpec((1, *rest), lambda i: (layer, *zeros))


def block(dtype=jnp.bfloat16, rows=BLOCK):
    return jax.ShapeDtypeStruct((rows, D), dtype)


def shards(
    frames_in,
    frame_time,
    cond_count,
    ln1_gain,
    ln1_bias,
    qkv_weight,
    qkv_bias,
    out_weight,
    out_bias,
    ln2_gain,
    ln2_bias,
    fc1_weight,
    fc1_bias,
    fc2_weight,
    fc2_bias,
):
    part = lax.axis_index("tm")
    pos = lax.axis_index("tensor")
    x, k = pos // 2, pos % 2

    def shift(array, s):
        pairs = [(t, ((t // 2 + s) % NX) * 2 + t % 2) for t in range(2 * NX)]
        return lax.ppermute(array, "tensor", pairs)

    def swap(array):
        return lax.ppermute(array, "tensor", [(t, t ^ 1) for t in range(2 * NX)])

    def spread(array):
        return [array] + [shift(array, -s) for s in (1, 2, 3)]

    def collect(parts):
        return [parts[0]] + [shift(parts[s], s) for s in (1, 2, 3)]

    mine = (k == (part // 4) % 2).astype(jnp.int32)
    idx = jnp.stack([x, k, mine]).astype(jnp.int32)
    times = jnp.repeat(frame_time, 2)
    far = jnp.int32(1 << 20)
    slot_ok = (jnp.arange(PARTS, dtype=jnp.int32) % 2) < jnp.repeat(cond_count, 2)
    patch_time = jnp.repeat(times, 32)
    key_time = jnp.concatenate(
        [patch_time, patch_time, jnp.where(slot_ok, times, far), jnp.full((KEYS - 2080,), far)]
    )[None, :]
    part_time = jnp.broadcast_to(times[:, None], (PARTS, 128))

    qkv_par = swap(qkv_weight)
    small = jnp.concatenate([qkv_bias.reshape(LAYERS, -1), fc1_bias], axis=1)
    small_par = swap(small)
    out_par = swap(out_weight)
    fc1_par = swap(fc1_weight)
    fc2_par = swap(fc2_weight)
    qkv_bias_par = small_par[:, : 3 * 128].reshape(LAYERS, 3, 128)
    fc1_bias_par = small_par[:, 3 * 128 :]

    call = functools.partial(
        pl.pallas_call, compiler_params=pltpu.CompilerParams(vmem_limit_bytes=48 << 20)
    )
    *normed, stream = call(
        prep_kernel,
        out_shape=[block()] * 5,
        in_specs=[SMEM, VMEM, VMEM, VMEM],
        out_specs=[VMEM] * 5,
    )(idx, frames_in[0].reshape(CLIPS, SLOTS, D), ln1_gain, ln1_bias)

    for layer in range(LAYERS):
        message = call(
            qkv_kernel,
            grid=(1,),
            out_shape=jax.ShapeDtypeStruct((PARTS, 56, 128), jnp.bfloat16),
            in_specs=[SMEM]
            + [VMEM] * 4
            + [of_layer(layer, a) for a in (qkv_weight, qkv_par, qkv_bias, qkv_bias_par)],
            out_specs=VMEM,
            scratch_shapes=[pltpu.VMEM((NX * PAD, D), jnp.bfloat16)],
        )(idx, *normed, qkv_weight, qkv_par, qkv_bias, qkv_bias_par)
        arrived = lax.all_to_all(message, "tm", 0, 0, tiled=True)
        arrived_par = swap(arrived)
        mixed = call(
            attn_kernel,
            out_shape=jax.ShapeDtypeStruct((PARTS, 24, 128), jnp.bfloat16),
            in_specs=[SMEM, SMEM] + [VMEM] * 4,
            out_specs=VMEM,
            scratch_shapes=[
                pltpu.VMEM((KEYS, 128), jnp.bfloat16),
                pltpu.VMEM((256, KEYS), jnp.float32),
                pltpu.VMEM((256, KEYS), jnp.bfloat16),
                pltpu.VMEM((256, 128), jnp.float32),
            ],
        )(idx, times, arrived, arrived_par, key_time, part_time)
        back = lax.all_to_all(mixed, "tm", 0, 0, tiled=True)
        partial = call(
            out_kernel,
            grid=(1,),
            out_shape=[block()] * 4,
            in_specs=[SMEM, VMEM, of_layer(layer, out_weight), of_layer(layer, out_par)],
            out_specs=[VMEM] * 4,
            scratch_shapes=[pltpu.VMEM((NX * PAD, 128), jnp.bfloat16)] * 2,
        )(idx, back, out_weight, out_par)
        first, normed_two = call(
            functools.partial(mid_kernel, layer),
            out_shape=[block(jnp.float32), block()],
            in_specs=[VMEM] * 8,
            out_specs=[VMEM] * 2,
        )(stream, *collect(partial), out_bias, ln2_gain, ln2_bias)
        partial = call(
            mlp_kernel,
            grid=(1,),
            out_shape=[block()] * 4,
            in_specs=[VMEM] * 4
            + [of_layer(layer, a) for a in (fc1_weight, fc1_par)]
            + [VMEM] * 2
            + [of_layer(layer, a) for a in (fc2_weight, fc2_par)],
            out_specs=[VMEM] * 4,
            scratch_shapes=[pltpu.VMEM((NX * PAD, D), jnp.bfloat16)],
        )(
            *spread(normed_two),
            fc1_weight,
            fc1_par,
            fc1_bias[layer : layer + 1],
            fc1_bias_par[layer : layer + 1],
            fc2_weight,
            fc2_par,
        )
        if layer + 1 < LAYERS:
            stream, ahead = call(
                functools.partial(end_kernel, layer),
                out_shape=[block()] * 2,
                in_specs=[VMEM] * 8,
                out_specs=[VMEM] * 2,
            )(first, *collect(partial), fc2_bias, ln1_gain, ln1_bias)
            normed = spread(ahead)
    stream, send = call(
        functools.partial(last_kernel, LAYERS - 1),
        out_shape=[block(), block(rows=32)],
        in_specs=[SMEM] + [VMEM] * 6,
        out_specs=[VMEM] * 2,
    )(idx, first, *collect(partial), fc2_bias)
    return call(
        place_kernel,
        out_shape=jax.ShapeDtypeStruct((1, BLOCK, D), jnp.bfloat16),
        in_specs=[SMEM] + [VMEM] * 2,
        out_specs=VMEM,
    )(idx, stream, swap(send))


def solution(mesh):
    in_specs = (
        P("tm", None, None),
        P(),
        P(),
        P(),
        P(),
        P(None, None, None, "tensor"),
        P(None, None, "tensor"),
        P(None, "tensor", None),
        P(),
        P(),
        P(),
        P(None, None, "tensor"),
        P(None, "tensor"),
        P(None, "tensor", None),
        P(),
    )
    out_specs = P("tm", "tensor", None)
    return jax.shard_map(shards, mesh=mesh, in_specs=in_specs, out_specs=out_specs, check_vma=False)
```

```python
import functools

import jax
import jax.numpy as jnp
from jax import lax
from jax.experimental import pallas as pl
from jax.experimental.pallas import tpu as pltpu
from jax.sharding import PartitionSpec as P

D = 1024
LAYERS = 2
PARTS = 32
FRAMES = 16
BLOCK = 65
PAD = 72
KEYS = 2176
NX = 4
HELD = 1032
LOG2E = 1.4426950408889634
SCALE = 0.125 * LOG2E
NEG = -1e30


def lanes(shape):
    return lax.broadcasted_iota(jnp.int32, shape, len(shape) - 1)


def subs(shape):
    return lax.broadcasted_iota(jnp.int32, shape, len(shape) - 2)


def norm(rows, gain, bias):
    center = jnp.mean(rows, axis=-1, keepdims=True)
    off = rows - center
    spread = jnp.mean(off * off, axis=-1, keepdims=True)
    return off * lax.rsqrt(spread + 1e-06) * gain + bias


def pack_kernel(w, bias, wo, out):
    for i in range(3):
        out[i, 0:D, :] = w[0, i]
        row = bias[1, i : i + 1, :]
        high = row.astype(jnp.bfloat16).astype(jnp.float32)
        middle = (row - high).astype(jnp.bfloat16).astype(jnp.float32)
        lowest = (row - high) - middle
        sub = subs((8, 128))
        tail = jnp.where(sub == 0, high, jnp.where(sub == 1, middle, jnp.where(sub == 2, lowest, 0.0)))
        out[i, D:HELD, :] = tail.astype(jnp.bfloat16)
    for j in range(8):
        out[3, 128 * j : 128 * j + 128, :] = wo[0, :, 128 * j : 128 * j + 128]
    out[3, D:HELD, :] = jnp.zeros((8, 128), jnp.bfloat16)


def tables_kernel(frame_time, cond_count, order, mask, row_time):
    for f in range(FRAMES):
        order[frame_time[f]] = f
    slot_time = jnp.full((FRAMES, 128), FRAMES, jnp.int32)
    times = jnp.zeros((PARTS, 128), jnp.int32)
    for g in range(PARTS):
        time = frame_time[g // 2]
        seen = jnp.where(g % 2 < cond_count[g // 2], time, FRAMES)
        slot_time = jnp.where(lanes(slot_time.shape) == g, seen, slot_time)
        times = jnp.where(subs(times.shape) == g, time, times)
    row_time[...] = times
    mask[:, 0:128] = jnp.where(slot_time <= subs(slot_time.shape), 0.0, NEG).astype(jnp.bfloat16)
    for t in range(FRAMES):
        seen = jnp.where(subs((FRAMES, 128)) >= t, 0.0, NEG)
        mask[:, 128 * t + 128 : 128 * t + 256] = seen.astype(jnp.bfloat16)


def from_row(ref, base, off, count):
    return pltpu.roll(ref[pl.ds(pl.multiple_of(base, 8), count), :], lax.rem(count - off, count), 0)


def prep_kernel(idx, x_ref, g_ref, b_ref, n0, n1, n2, n3, own, wide):
    x, k = idx[0], idx[1]
    gain, bias = g_ref[0:1, :], b_ref[0:1, :]
    wide[...] = x_ref[0].astype(jnp.float32)
    for s, out in enumerate((n0, n1, n2, n3)):
        chip = lax.rem(x + s, NX)
        for b in range(2):
            rows = from_row(wide, 64 * (2 * chip + b) + 32 * k, 2 * chip + b, 40)[:32]
            out[32 * b : 32 * b + 32, :] = norm(rows, gain, bias).astype(jnp.bfloat16)
            if s == 0:
                own[32 * b : 32 * b + 32, :] = rows.astype(jnp.bfloat16)
        rows = from_row(wide, 64 * (2 * chip + k) + 64, 2 * chip + k, 8)[:1]
        out[64:65, :] = norm(rows, gain, bias).astype(jnp.bfloat16)
        if s == 0:
            own[64:65, :] = rows.astype(jnp.bfloat16)


def emit(out, w, biases, rows, places, tails):
    count = rows.shape[0]
    low = lanes((count, 128)) < 64
    low8 = lanes((8, 128)) < 64
    sub = lax.broadcasted_iota(jnp.int32, (8, 128), 0)
    q, key, val = (
        jnp.dot(rows[...], w[i, 0:D, :], preferred_element_type=jnp.float32) + biases[i]
        for i in range(3)
    )
    q_r, key_r, val_r = (pltpu.roll(a, 64, 1) for a in (q, key, val))
    for hl in range(2):
        if hl == 0:
            kv = jnp.where(low, key, val_r)
            q_lo, q_hi = q, q_r
        else:
            kv = jnp.where(low, key_r, val)
            q_lo, q_hi = q_r, q
        for slot, at in places:
            out[slot + hl, 0:32, :] = kv[at : at + 32].astype(jnp.bfloat16)
            out[slot + hl, 32:48, :] = jnp.where(
                low[:16], q_lo[at : at + 16], q_hi[at + 16 : at + 32]
            ).astype(jnp.bfloat16)
            out[slot + hl, 48:56, :] = jnp.zeros((8, 128), jnp.bfloat16)
        for slot, at in tails:
            tail = jnp.where(
                sub == 0,
                jnp.broadcast_to(kv[at : at + 1], (8, 128)),
                jnp.where((sub == 1) & low8, jnp.broadcast_to(q_lo[at : at + 1], (8, 128)), 0.0),
            )
            out[slot + hl, 48:56, :] = tail.astype(jnp.bfloat16)


def qkv_kernel(idx, n0, n1, n2, n3, w_own, w_par, b_own, b_par, out, rows):
    k = idx[1]
    for s, n in enumerate((n0, n1, n2, n3)):
        rows[72 * s : 72 * s + 65, :] = n[...]
    for w, bias, side in ((w_own, b_own, k), (w_par, b_par, 1 - k)):
        places = [(s * 8 + b * 4 + 2 * side, 72 * s + 32 * b) for s in range(NX) for b in range(2)]
        tails = [(s * 8 + k * 4 + 2 * side, 72 * s + 64) for s in range(NX)]
        emit(out, w.at[0], [bias[0, i : i + 1, :] for i in range(3)], rows, places, tails)


def turn_kernel(idx, first, y0, y1, y2, y3, o_bias, gain, bias, *rest):
    owns, pars, (stream, out, rows) = rest[:NX], rest[NX : 2 * NX], rest[2 * NX :]
    k = idx[1]
    summed = (y0[...].astype(jnp.float32) + y1[...].astype(jnp.float32)) + (
        y2[...].astype(jnp.float32) + y3[...].astype(jnp.float32)
    )
    new = (first[...] + summed + o_bias[0:1, :]).astype(jnp.bfloat16)
    stream[...] = new
    rows[0:65, :] = norm(new.astype(jnp.float32), gain[1:2, :], bias[1:2, :]).astype(jnp.bfloat16)
    for s in range(NX):
        for w, side in ((owns[s], k), (pars[s], 1 - k)):
            places = [(b * 16 + s * 4 + 2 * side, 32 * b) for b in range(2)]
            biases = [jnp.sum(w[i, D:HELD, :].astype(jnp.float32), axis=0, keepdims=True) for i in range(3)]
            emit(out, w, biases, rows, places, [(k * 16 + s * 4 + 2 * side, 64)])


def attn_kernel(layer, idx, order, mask, part_time, r_own, r_par, out, kt, vals, score, prob):
    mine = idx[2 + layer]
    low = lanes((128, 128)) < 64

    def place(at, block):
        key, val = block.astype(jnp.float32), block
        both = jnp.where(low, key, pltpu.roll(key, 64, 1))
        kt[0:128, at : at + 128] = both.T.astype(jnp.bfloat16)
        vals[at : at + 128, :] = jnp.where(low, jnp.ones_like(val), val)

    def queries(packed, which):
        scaled = packed * SCALE
        high = scaled.astype(jnp.bfloat16).astype(jnp.float32)
        rest = scaled - high
        left = jnp.where(lanes(packed.shape) < 64, high, pltpu.roll(rest, 64, 1))
        return jnp.concatenate([left.astype(jnp.bfloat16), which.astype(jnp.bfloat16)], axis=1)

    sub = lax.broadcasted_iota(jnp.int32, (PARTS, 8, 128), 1)
    tail_own = r_own[:, 48:56, :].astype(jnp.float32)
    tail_par = r_par[:, 48:56, :].astype(jnp.float32)
    extra = jnp.sum(jnp.where(sub == 0, jnp.where(mine == 1, tail_own, tail_par), 0.0), axis=1)
    place(0, jnp.concatenate([extra, jnp.zeros((96, 128), jnp.float32)], axis=0).astype(jnp.bfloat16))
    kt[128:144, :] = mask[...]
    kt[144:256, :] = jnp.zeros((112, KEYS), jnp.bfloat16)
    for t in range(FRAMES):
        at = pl.ds(2 * order[t], 2)
        own = r_own[at, 0:32, :].reshape(64, 128)
        par = r_par[at, 0:32, :].reshape(64, 128)
        place(128 * t + 128, jnp.concatenate([own, par], axis=0))

    def attend(lhs, rows, n, buf):
        score[buf, 0:rows, 0:n] = jnp.dot(lhs, kt[:, 0:n], preferred_element_type=jnp.float32)
        for r in range(0, rows, 16):
            now = score[buf, r : r + 16, 0:n]
            now = jnp.exp2(now - jnp.max(now, axis=1, keepdims=True))
            prob[buf, r : r + 16, 0:n] = now.astype(jnp.bfloat16)
        mixed = jnp.dot(prob[buf, 0:rows, 0:n], vals[0:n, :], preferred_element_type=jnp.float32)
        return mixed / pltpu.roll(mixed, 64, 1)

    row = lax.broadcasted_iota(jnp.int32, (256, 128), 0)
    for i in range(4):
        packed = jnp.concatenate(
            [r_own[pl.ds(2 * order[4 * i + t], 2), 32:48, :].reshape(32, 128) for t in range(4)], axis=0
        ).astype(jnp.float32)
        packed = jnp.concatenate([packed, pltpu.roll(packed, 64, 1)], axis=0)
        which = jnp.where(lanes((256, 128)) == 4 * i + (row % 128) // 32, 1.0, 0.0)
        res = attend(queries(packed, which), 256, 128 + 512 * (i + 1), i % 2)
        merged = jnp.where(low, pltpu.roll(res[:128], 64, 1), res[128:]).astype(jnp.bfloat16)
        for t in range(4):
            out[pl.ds(2 * order[4 * i + t], 2), 0:16, :] = merged[32 * t : 32 * t + 32].reshape(2, 16, 128)
    packed = jnp.sum(jnp.where(sub == 1, tail_own, 0.0), axis=1)
    which = jnp.where(lanes((PARTS, 128)) == part_time[...], 1.0, 0.0)
    res = pltpu.roll(attend(queries(packed, which), PARTS, KEYS, 0), 64, 1)
    out[:, 16:24, :] = jnp.broadcast_to(res[:, None, :], (PARTS, 8, 128)).astype(jnp.bfloat16)


def pair(first, second):
    low = lanes((24, 128)) < 64
    first, second = first.astype(jnp.float32), second.astype(jnp.float32)
    return (
        jnp.where(low, first, pltpu.roll(second, 64, 1)).astype(jnp.bfloat16),
        jnp.where(low, pltpu.roll(first, 64, 1), second).astype(jnp.bfloat16),
    )


def gather_heads(dst, at, back, patches, tail):
    for b, slot in enumerate(patches):
        lo, hi = pair(back[slot], back[slot + 1])
        dst[at + 32 * b : at + 32 * b + 16, :] = lo[:16]
        dst[at + 32 * b + 16 : at + 32 * b + 32, :] = hi[:16]
    lo, _ = pair(back[tail], back[tail + 1])
    dst[at + 64 : at + 72, :] = lo[16:24]


def out_kernel(idx, back, w_own, w_par, p0, p1, p2, p3, left, right):
    k = idx[1]
    for dst, side in ((left, k), (right, 1 - k)):
        for s in range(NX):
            slots = [s * 8 + b * 4 + 2 * side for b in range(2)]
            gather_heads(dst, 72 * s, back, slots, s * 8 + k * 4 + 2 * side)
    for j in range(4):
        cols = slice(256 * j, 256 * j + 256)
        partial = jnp.dot(left[...], w_own[0, :, cols], preferred_element_type=jnp.float32) + jnp.dot(
            right[...], w_par[0, :, cols], preferred_element_type=jnp.float32
        )
        for s, out in enumerate((p0, p1, p2, p3)):
            out[:, cols] = partial[72 * s : 72 * s + 65].astype(jnp.bfloat16)


def w_out(w):
    return jnp.concatenate([w[3, 128 * j : 128 * j + 128, :] for j in range(8)], axis=1)


def whole_out_kernel(idx, back, own, o_bias, gain, bias, *rest):
    owns, pars, (first, normed, heads) = rest[:NX], rest[NX : 2 * NX], rest[2 * NX :]
    k = idx[1]
    total = None
    for s in range(NX):
        for c, (w, side) in enumerate(((owns[s], k), (pars[s], 1 - k))):
            base = s * 4 + 2 * side
            gather_heads(heads.at[2 * s + c], 0, back, [base, 16 + base], k * 16 + base)
            part = jnp.dot(heads[2 * s + c], w_out(w), preferred_element_type=jnp.float32)
            total = part if total is None else total + part
    rows = own[...].astype(jnp.float32) + total[:65] + o_bias[1:2, :]
    first[...] = rows
    normed[...] = norm(rows, gain[1:2, :], bias[1:2, :]).astype(jnp.bfloat16)


def mid_kernel(layer, own, p0, p1, p2, p3, o_bias, gain, bias, first, normed):
    rows = own[...].astype(jnp.float32)
    summed = (p0[...].astype(jnp.float32) + p1[...].astype(jnp.float32)) + (
        p2[...].astype(jnp.float32) + p3[...].astype(jnp.float32)
    )
    rows = rows + summed + o_bias[layer : layer + 1, :]
    first[...] = rows
    normed[...] = norm(rows, gain[layer : layer + 1, :], bias[layer : layer + 1, :]).astype(jnp.bfloat16)


def mlp_kernel(layer, n, w1_own, w1_par, b1_own, b1_par, w2_own, w2_par, y, rows):
    rows[0:65, :] = n[...]
    total = None
    for w1, b1, w2 in ((w1_own, b1_own, w2_own), (w1_par, b1_par, w2_par)):
        inner = jnp.dot(rows[...], w1[layer], preferred_element_type=jnp.float32) + b1[layer : layer + 1, :]
        inner = (0.5 * inner * (1.0 + lax.erf(inner * 0.7071067811865476))).astype(jnp.bfloat16)
        part = jnp.dot(inner, w2[layer], preferred_element_type=jnp.float32)
        total = part if total is None else total + part
    y[...] = total[:65].astype(jnp.bfloat16)


def last_kernel(layer, idx, first, y0, y1, y2, y3, o_bias, stream, send):
    k = idx[1]
    summed = (y0[...].astype(jnp.float32) + y1[...].astype(jnp.float32)) + (
        y2[...].astype(jnp.float32) + y3[...].astype(jnp.float32)
    )
    rows = (first[...] + summed + o_bias[layer : layer + 1, :]).astype(jnp.bfloat16)
    stream[...] = rows
    send[...] = jnp.where(k == 0, rows[32:64], rows[0:32])


def place_kernel(idx, stream, recv, out):
    k = idx[1]
    out[0, 0:32, :] = jnp.where(k == 0, stream[0:32, :], recv[...])
    out[0, 32:64, :] = jnp.where(k == 0, recv[...], stream[32:64, :])
    out[0, 64:65, :] = stream[64:65, :]


VMEM = pl.BlockSpec(memory_space=pltpu.VMEM)
SMEM = pl.BlockSpec(memory_space=pltpu.SMEM)


def block(dtype=jnp.bfloat16, rows=BLOCK):
    return jax.ShapeDtypeStruct((rows, D), dtype)


def call(kernel, args, out_shape, scratch=(), scalars=1, limit=24, out_specs=None):
    return pl.pallas_call(
        kernel,
        out_shape=out_shape,
        in_specs=[SMEM] * scalars + [VMEM] * (len(args) - scalars),
        out_specs=out_specs or ([VMEM] * len(out_shape) if isinstance(out_shape, list) else VMEM),
        scratch_shapes=list(scratch),
        compiler_params=pltpu.CompilerParams(vmem_limit_bytes=limit << 20),
    )(*args)


def of_layer(layer, array):
    rest = array.shape[1:]
    zeros = (0,) * len(rest)
    return pl.BlockSpec((1, *rest), lambda i: (layer, *zeros))


def shards(
    frames_in,
    frame_time,
    cond_count,
    ln1_gain,
    ln1_bias,
    qkv_weight,
    qkv_bias,
    out_weight,
    out_bias,
    ln2_gain,
    ln2_bias,
    fc1_weight,
    fc1_bias,
    fc2_weight,
    fc2_bias,
):
    part = lax.axis_index("tm")
    pos = lax.axis_index("tensor")
    x, k = pos // 2, pos % 2

    def shift(array, s):
        pairs = [(t, ((t // 2 + s) % NX) * 2 + t % 2) for t in range(2 * NX)]
        return lax.ppermute(array, "tensor", pairs)

    def swap(array):
        return lax.ppermute(array, "tensor", [(t, t ^ 1) for t in range(2 * NX)])

    def spread(array):
        return [array] + [shift(array, -s) for s in (1, 2, 3)]

    def collect(parts):
        return [parts[0]] + [shift(parts[s], s) for s in (1, 2, 3)]

    tie = lax.optimization_barrier

    def attention(layer, message, *late):
        arrived = lax.all_to_all(message, "tm", 0, 0, tiled=True)
        arrived, *late = tie((arrived, *late))
        arrived_par = swap(arrived)
        arrived, arrived_par, *late = tie((arrived, arrived_par, *late))
        late = [swap(a) for a in late]
        mixed = call(
            functools.partial(attn_kernel, layer),
            (idx, order, mask, row_time, arrived, arrived_par),
            jax.ShapeDtypeStruct((PARTS, 24, 128), jnp.bfloat16),
            [
                pltpu.VMEM((256, KEYS), jnp.bfloat16),
                pltpu.VMEM((KEYS, 128), jnp.bfloat16),
                pltpu.VMEM((2, 256, KEYS), jnp.float32),
                pltpu.VMEM((2, 256, KEYS), jnp.bfloat16),
            ],
            scalars=2,
        )
        mixed, *late = tie((mixed, *late))
        back = lax.all_to_all(mixed, "tm", 0, 0, tiled=True)
        return tie((back, *late))

    message_shape = jax.ShapeDtypeStruct((PARTS, 56, 128), jnp.bfloat16)

    def mlp(layer, blocks):
        outs = []
        for n in blocks:
            outs.append(
                call(
                    functools.partial(mlp_kernel, layer),
                    (n, fc1_weight, fc1_par, fc1_bias, fc1_bias_par, fc2_weight, fc2_par),
                    block(),
                    [pltpu.VMEM((PAD, D), jnp.bfloat16)],
                    scalars=0,
                )
            )
        return outs

    qkv_par = swap(qkv_weight)
    qkv_bias_par = swap(qkv_bias)
    idx = jnp.stack([x, k, k == (part // 4) % 2, k == part // 16]).astype(jnp.int32)
    held = pl.pallas_call(
        pack_kernel,
        grid=(1,),
        out_shape=jax.ShapeDtypeStruct((4, HELD, 128), jnp.bfloat16),
        in_specs=[of_layer(1, qkv_weight), VMEM, of_layer(1, out_weight)],
        out_specs=VMEM,
        compiler_params=pltpu.CompilerParams(vmem_limit_bytes=8 << 20),
    )(qkv_weight, qkv_bias, out_weight)
    helds = spread(held)
    order, mask, row_time = call(
        tables_kernel,
        (frame_time, cond_count),
        [
            jax.ShapeDtypeStruct((FRAMES,), jnp.int32),
            jax.ShapeDtypeStruct((FRAMES, KEYS), jnp.bfloat16),
            jax.ShapeDtypeStruct((PARTS, 128), jnp.int32),
        ],
        scalars=2,
        out_specs=[SMEM, VMEM, VMEM],
    )
    *normed, stream = call(
        prep_kernel,
        (idx, frames_in, ln1_gain, ln1_bias),
        [block()] * 5,
        [pltpu.VMEM((8 * BLOCK, D), jnp.float32)],
    )
    qkv_par, qkv_bias_par, order, mask, row_time, w2, idx, *normed = tie(
        (qkv_par, qkv_bias_par, order, mask, row_time, fc2_weight, idx, *normed)
    )
    fc2_par = swap(w2)
    message = call(
        qkv_kernel,
        (idx, *normed, qkv_weight, qkv_par, qkv_bias, qkv_bias_par),
        message_shape,
        [pltpu.VMEM((NX * PAD, D), jnp.bfloat16)],
    )
    message, fc2_par = tie((message, fc2_par))
    back, out_par, fc1_par, fc1_bias_par, held_par = attention(
        0, message, out_weight, fc1_weight, fc1_bias, held
    )
    partial = pl.pallas_call(
        out_kernel,
        grid=(1,),
        out_shape=[block()] * 4,
        in_specs=[SMEM, VMEM, of_layer(0, out_weight), of_layer(0, out_par)],
        out_specs=[VMEM] * 4,
        scratch_shapes=[pltpu.VMEM((NX * PAD, 128), jnp.bfloat16)] * 2,
        compiler_params=pltpu.CompilerParams(vmem_limit_bytes=12 << 20),
    )(idx, back, out_weight, out_par)
    partial = collect(partial)
    first, normed_two = call(
        functools.partial(mid_kernel, 0),
        (stream, *partial, out_bias, ln2_gain, ln2_bias),
        [block(jnp.float32), block()],
        scalars=0,
    )
    partial = mlp(0, spread(normed_two))
    partial = collect(partial)
    held_pars = [held_par] + [swap(helds[s]) for s in (1, 2, 3)]
    stream, message = call(
        turn_kernel,
        (idx, first, *partial, fc2_bias, ln1_gain, ln1_bias, *helds, *held_pars),
        [block(), message_shape],
        [pltpu.VMEM((PAD, D), jnp.bfloat16)],
    )
    (back,) = attention(1, message)
    first, normed_two = call(
        whole_out_kernel,
        (idx, back, stream, out_bias, ln2_gain, ln2_bias, *helds, *held_pars),
        [block(jnp.float32), block()],
        [pltpu.VMEM((2 * NX, PAD, 128), jnp.bfloat16)],
    )
    partial = mlp(1, spread(normed_two))
    partial = collect(partial)
    stream, send = call(
        functools.partial(last_kernel, LAYERS - 1),
        (idx, first, *partial, fc2_bias),
        [block(), block(rows=32)],
    )
    recv = swap(send)
    return call(place_kernel, (idx, stream, recv), jax.ShapeDtypeStruct((1, BLOCK, D), jnp.bfloat16))


def solution(mesh):
    in_specs = (
        P("tm", None, None),
        P(),
        P(),
        P(),
        P(),
        P(None, None, None, "tensor"),
        P(None, None, "tensor"),
        P(None, "tensor", None),
        P(),
        P(),
        P(),
        P(None, None, "tensor"),
        P(None, "tensor"),
        P(None, "tensor", None),
        P(),
    )
    out_specs = P("tm", "tensor", None)
    return jax.shard_map(shards, mesh=mesh, in_specs=in_specs, out_specs=out_specs, check_vma=False)
```

```python
import functools

import jax
import jax.numpy as jnp
from jax import lax
from jax.experimental import pallas as pl
from jax.experimental.pallas import tpu as pltpu
from jax.sharding import PartitionSpec as P

D = 1024
LAYERS = 2
PARTS = 32
FRAMES = 16
BLOCK = 65
PAD = 72
KEYS = 2176
NX = 4
HELD = 1032
LOG2E = 1.4426950408889634
SCALE = 0.125 * LOG2E
NEG = -1e30

GROUPS = ((0,), (1, 3), (2,))


def lanes(shape):
    return lax.broadcasted_iota(jnp.int32, shape, len(shape) - 1)


def subs(shape):
    return lax.broadcasted_iota(jnp.int32, shape, len(shape) - 2)


def norm(rows, gain, bias):
    center = jnp.mean(rows, axis=-1, keepdims=True)
    off = rows - center
    spread = jnp.mean(off * off, axis=-1, keepdims=True)
    return off * lax.rsqrt(spread + 1e-06) * gain + bias


def tables_kernel(frame_time, cond_count, w1_ref, b1_ref, w2_ref, order, mask, row_time, packed, bias, sems):
    copies = [
        pltpu.make_async_copy(w1_ref.at[1], packed.at[0, 0:D], sems.at[0]),
        pltpu.make_async_copy(w2_ref.at[1, :, 0:512], packed.at[1, 0:512], sems.at[1]),
        pltpu.make_async_copy(w2_ref.at[1, :, 512:D], packed.at[1, 512:D], sems.at[2]),
        pltpu.make_async_copy(b1_ref, bias, sems.at[3]),
    ]
    for copy in copies:
        copy.start()
    for f in range(FRAMES):
        order[frame_time[f]] = f
    slot_time = jnp.full((FRAMES, 128), FRAMES, jnp.int32)
    times = jnp.zeros((PARTS, 128), jnp.int32)
    for g in range(PARTS):
        time = frame_time[g // 2]
        seen = jnp.where(g % 2 < cond_count[g // 2], time, FRAMES)
        slot_time = jnp.where(lanes(slot_time.shape) == g, seen, slot_time)
        times = jnp.where(subs(times.shape) == g, time, times)
    row_time[...] = times
    mask[:, 0:128] = jnp.where(slot_time <= subs(slot_time.shape), 0.0, NEG).astype(jnp.bfloat16)
    for t in range(FRAMES):
        seen = jnp.where(subs((FRAMES, 128)) >= t, 0.0, NEG)
        mask[:, 128 * t + 128 : 128 * t + 256] = seen.astype(jnp.bfloat16)
    for copy in copies:
        copy.wait()
    packed[0, D:HELD, :] = split_rows(bias[1:2, :])
    packed[1, D:HELD, :] = jnp.zeros((8, 512), jnp.bfloat16)


def split_rows(row):
    high = row.astype(jnp.bfloat16).astype(jnp.float32)
    middle = (row - high).astype(jnp.bfloat16).astype(jnp.float32)
    lowest = (row - high) - middle
    sub = subs((8, row.shape[1]))
    rows = jnp.where(sub == 0, high, jnp.where(sub == 1, middle, jnp.where(sub == 2, lowest, 0.0)))
    return rows.astype(jnp.bfloat16)


def from_row(ref, base, off, count):
    return pltpu.roll(ref[pl.ds(pl.multiple_of(base, 8), count), :], lax.rem(count - off, count), 0)


def emit(out, q, key, val, places, tails):
    low = lanes(q.shape) < 64
    low8 = lanes((8, 128)) < 64
    sub = lax.broadcasted_iota(jnp.int32, (8, 128), 0)
    q_r, key_r, val_r = (pltpu.roll(a, 64, 1) for a in (q, key, val))
    for hl in range(2):
        if hl == 0:
            kv = jnp.where(low, key, val_r)
            q_lo, q_hi = q, q_r
        else:
            kv = jnp.where(low, key_r, val)
            q_lo, q_hi = q_r, q
        for slot, at in places:
            out[slot + hl, 0:32, :] = kv[at : at + 32].astype(jnp.bfloat16)
            out[slot + hl, 32:48, :] = jnp.where(
                low[:16], q_lo[at : at + 16], q_hi[at + 16 : at + 32]
            ).astype(jnp.bfloat16)
            out[slot + hl, 48:56, :] = jnp.zeros((8, 128), jnp.bfloat16)
        for slot, at in tails:
            tail = jnp.where(
                sub == 0,
                jnp.broadcast_to(kv[at : at + 1], (8, 128)),
                jnp.where((sub == 1) & low8, jnp.broadcast_to(q_lo[at : at + 1], (8, 128)), 0.0),
            )
            out[slot + hl, 48:56, :] = tail.astype(jnp.bfloat16)


def start_kernel(
    idx, x_ref, w_ref, wo_ref, bias_ref, g_ref, b_ref, rows, own, out, held, raw, wide, w, biases, norms, sems
):
    x, k = idx[0], idx[1]
    copies = [
        pltpu.make_async_copy(x_ref.at[0], raw, sems.at[0]),
        pltpu.make_async_copy(w_ref.at[0, 0], w.at[0], sems.at[1]),
        pltpu.make_async_copy(w_ref.at[0, 1], w.at[1], sems.at[2]),
        pltpu.make_async_copy(w_ref.at[0, 2], w.at[2], sems.at[15]),
        pltpu.make_async_copy(bias_ref, biases, sems.at[14]),
        pltpu.make_async_copy(w_ref.at[1], held.at[0:3, 0:D, :], sems.at[3]),
    ]
    for j in range(8):
        cols = slice(128 * j, 128 * j + 128)
        copies.append(pltpu.make_async_copy(wo_ref.at[1, :, cols], held.at[3, cols, :], sems.at[4 + j]))
    first = [
        pltpu.make_async_copy(g_ref, norms.at[0], sems.at[12]),
        pltpu.make_async_copy(b_ref, norms.at[1], sems.at[13]),
    ]
    for copy in first + copies:
        copy.start()
    copies[0].wait()
    wide[...] = raw[...].astype(jnp.float32)
    for copy in first:
        copy.wait()
    gain, bias = norms[0, 0:1, :], norms[1, 0:1, :]
    for s in range(NX):
        chip = lax.rem(x + s, NX)
        for b in range(2):
            part = from_row(wide, 64 * (2 * chip + b) + 32 * k, 2 * chip + b, 40)[:32]
            at = PAD * s + 32 * b
            rows[at : at + 32, :] = norm(part, gain, bias).astype(jnp.bfloat16)
            if s == 0:
                own[32 * b : 32 * b + 32, :] = part.astype(jnp.bfloat16)
        part = from_row(wide, 64 * (2 * chip + k) + 64, 2 * chip + k, 8)
        rows[PAD * s + 64 : PAD * s + 72, :] = norm(part, gain, bias).astype(jnp.bfloat16)
        if s == 0:
            own[64:65, :] = part[:1].astype(jnp.bfloat16)
    copies[4].wait()
    heads_of(k, k, rows, w, biases, out, copies[1:4])
    for copy in copies[5:]:
        copy.wait()
    for i in range(3):
        held[i, D:HELD, :] = split_rows(biases[i, 1:2, :])
    held[3, D:HELD, :] = jnp.zeros((8, 128), jnp.bfloat16)


def heads_of(k, side, rows, w, biases, out, copies):
    places = [(s * 8 + b * 4 + 2 * side, 72 * s + 32 * b) for s in range(NX) for b in range(2)]
    tails = [(s * 8 + k * 4 + 2 * side, 72 * s + 64) for s in range(NX)]
    parts = []
    for i in range(3):
        copies[i].wait()
        parts.append(jnp.dot(rows[...], w[i], preferred_element_type=jnp.float32) + biases[i, 0:1, :])
    emit(out, *parts, places, tails)


def partner_kernel(idx, rows, w_ref, biases, other, out, w, sems):
    k = idx[1]
    copies = [pltpu.make_async_copy(w_ref.at[0, i], w.at[i], sems.at[i]) for i in range(3)]
    for copy in copies:
        copy.start()
    heads_of(k, 1 - k, rows, w, biases, out, copies)


def turn_kernel(idx, first, y0, y1, y2, y3, o_bias, gain, bias, *rest):
    owns, pars, (stream, out, rows, w, acc, sems) = rest[:NX], rest[NX : 2 * NX], rest[2 * NX :]
    k = idx[1]
    copies = [pltpu.make_async_copy(owns[s].at[0:3], w.at[s], sems.at[s]) for s in range(NX)]
    for copy in copies:
        copy.start()
    summed = (y0[...].astype(jnp.float32) + y1[...].astype(jnp.float32)) + (
        y2[...].astype(jnp.float32) + y3[...].astype(jnp.float32)
    )
    new = (first[...] + summed + o_bias[0:1, :]).astype(jnp.bfloat16)
    stream[...] = new
    rows[0:65, :] = norm(new.astype(jnp.float32), gain[1:2, :], bias[1:2, :]).astype(jnp.bfloat16)

    def project(c, weight):
        for i in range(3):
            bias_row = jnp.sum(weight[i, D:HELD, :].astype(jnp.float32), axis=0, keepdims=True)
            acc[c, i] = jnp.dot(rows[...], weight[i, 0:D, :], preferred_element_type=jnp.float32) + bias_row

    for s in range(NX):
        project(2 * s + 1, pars[s])

    def arrived(s, carry):
        pltpu.make_async_copy(owns[0].at[0:3], w.at[s], sems.at[s]).wait()
        project(2 * s, w.at[s])
        return carry

    lax.fori_loop(0, NX, arrived, 0)

    def one(c, carry):
        base = c // 2 * 4 + 2 * lax.rem(k + c, 2)
        emit(out, acc[c, 0], acc[c, 1], acc[c, 2], [(base, 0), (16 + base, 32)], [(k * 16 + base, 64)])
        return carry

    lax.fori_loop(0, 2 * NX, one, 0)


def attn_kernel(layer, idx, order, mask, part_time, r_own, r_par, out, kt, vals, score, prob):
    mine = idx[2 + layer]
    low = lanes((128, 128)) < 64

    def place(at, block):
        key, val = block.astype(jnp.float32), block
        both = jnp.where(low, key, pltpu.roll(key, 64, 1))
        kt[0:128, at : at + 128] = both.T.astype(jnp.bfloat16)
        vals[at : at + 128, :] = jnp.where(low, jnp.ones_like(val), val)

    def queries(packed, which):
        scaled = packed * SCALE
        high = scaled.astype(jnp.bfloat16).astype(jnp.float32)
        rest = scaled - high
        left = jnp.where(lanes(packed.shape) < 64, high, pltpu.roll(rest, 64, 1))
        return jnp.concatenate([left.astype(jnp.bfloat16), which.astype(jnp.bfloat16)], axis=1)

    sub = lax.broadcasted_iota(jnp.int32, (PARTS, 8, 128), 1)
    tail_own = r_own[:, 48:56, :].astype(jnp.float32)
    tail_par = r_par[:, 48:56, :].astype(jnp.float32)
    extra = jnp.sum(jnp.where(sub == 0, jnp.where(mine == 1, tail_own, tail_par), 0.0), axis=1)
    place(0, jnp.concatenate([extra, jnp.zeros((96, 128), jnp.float32)], axis=0).astype(jnp.bfloat16))
    kt[128:144, :] = mask[...]
    kt[144:256, :] = jnp.zeros((112, KEYS), jnp.bfloat16)
    for t in range(FRAMES):
        at = pl.ds(2 * order[t], 2)
        own = r_own[at, 0:32, :].reshape(64, 128)
        par = r_par[at, 0:32, :].reshape(64, 128)
        place(128 * t + 128, jnp.concatenate([own, par], axis=0))

    def attend(lhs, rows, n, buf):
        score[buf, 0:rows, 0:n] = jnp.dot(lhs, kt[:, 0:n], preferred_element_type=jnp.float32)
        for r in range(0, rows, 16):
            now = score[buf, r : r + 16, 0:n]
            now = jnp.exp2(now - jnp.max(now, axis=1, keepdims=True))
            prob[buf, r : r + 16, 0:n] = now.astype(jnp.bfloat16)
        mixed = jnp.dot(prob[buf, 0:rows, 0:n], vals[0:n, :], preferred_element_type=jnp.float32)
        return mixed / pltpu.roll(mixed, 64, 1)

    row = lax.broadcasted_iota(jnp.int32, (256, 128), 0)
    for i in range(4):
        packed = jnp.concatenate(
            [r_own[pl.ds(2 * order[4 * i + t], 2), 32:48, :].reshape(32, 128) for t in range(4)], axis=0
        ).astype(jnp.float32)
        packed = jnp.concatenate([packed, pltpu.roll(packed, 64, 1)], axis=0)
        which = jnp.where(lanes((256, 128)) == 4 * i + (row % 128) // 32, 1.0, 0.0)
        res = attend(queries(packed, which), 256, 128 + 512 * (i + 1), i % 2)
        merged = jnp.where(low, pltpu.roll(res[:128], 64, 1), res[128:]).astype(jnp.bfloat16)
        for t in range(4):
            out[pl.ds(2 * order[4 * i + t], 2), 0:16, :] = merged[32 * t : 32 * t + 32].reshape(2, 16, 128)
    packed = jnp.sum(jnp.where(sub == 1, tail_own, 0.0), axis=1)
    which = jnp.where(lanes((PARTS, 128)) == part_time[...], 1.0, 0.0)
    res = pltpu.roll(attend(queries(packed, which), PARTS, KEYS, 0), 64, 1)
    out[:, 16:24, :] = jnp.broadcast_to(res[:, None, :], (PARTS, 8, 128)).astype(jnp.bfloat16)


def pair(first, second):
    low = lanes((24, 128)) < 64
    first, second = first.astype(jnp.float32), second.astype(jnp.float32)
    return (
        jnp.where(low, first, pltpu.roll(second, 64, 1)).astype(jnp.bfloat16),
        jnp.where(low, pltpu.roll(first, 64, 1), second).astype(jnp.bfloat16),
    )


def gather_heads(dst, at, back, patches, tail):
    for b, slot in enumerate(patches):
        lo, hi = pair(back[slot], back[slot + 1])
        dst[at + 32 * b : at + 32 * b + 16, :] = lo[:16]
        dst[at + 32 * b + 16 : at + 32 * b + 32, :] = hi[:16]
    lo, _ = pair(back[tail], back[tail + 1])
    dst[at + 64 : at + 72, :] = lo[16:24]


def out_kernel(idx, back, w_own, w_par, p0, p1, p2, p3, left, right):
    k = idx[1]
    for dst, side in ((left, k), (right, 1 - k)):
        for s in range(NX):
            slots = [s * 8 + b * 4 + 2 * side for b in range(2)]
            gather_heads(dst, 72 * s, back, slots, s * 8 + k * 4 + 2 * side)
    for j in range(4):
        cols = slice(256 * j, 256 * j + 256)
        partial = jnp.dot(left[...], w_own[0, :, cols], preferred_element_type=jnp.float32) + jnp.dot(
            right[...], w_par[0, :, cols], preferred_element_type=jnp.float32
        )
        for s, out in enumerate((p0, p1, p2, p3)):
            out[:, cols] = partial[72 * s : 72 * s + 65].astype(jnp.bfloat16)


def mid_kernel(layer, own, p0, p1, p2, p3, o_bias, gain, bias, first, normed):
    rows = own[...].astype(jnp.float32)
    summed = (p0[...].astype(jnp.float32) + p1[...].astype(jnp.float32)) + (
        p2[...].astype(jnp.float32) + p3[...].astype(jnp.float32)
    )
    rows = rows + summed + o_bias[layer : layer + 1, :]
    first[...] = rows
    normed[...] = norm(rows, gain[layer : layer + 1, :], bias[layer : layer + 1, :]).astype(jnp.bfloat16)


def whole_out_kernel(idx, back, own, o_bias, gain, bias, *rest):
    owns, pars, (first, normed, heads, w, sems) = rest[:NX], rest[NX : 2 * NX], rest[2 * NX :]
    k = idx[1]
    copies = [pltpu.make_async_copy(owns[s].at[3, 0:D], w.at[s], sems.at[s]) for s in range(NX)]
    for copy in copies:
        copy.start()
    total = None
    for c, side in ((1, 1 - k), (0, k)):
        for s in range(NX):
            base = s * 4 + 2 * side
            gather_heads(heads.at[2 * s + c], 0, back, [base, 16 + base], k * 16 + base)
            if c == 0:
                copies[s].wait()
            source = w.at[s] if c == 0 else pars[s].at[3]
            weight = jnp.concatenate([source[128 * j : 128 * j + 128, :] for j in range(8)], axis=1)
            part = jnp.dot(heads[2 * s + c], weight, preferred_element_type=jnp.float32)
            total = part if total is None else total + part
    rows = own[...].astype(jnp.float32) + total[:65] + o_bias[1:2, :]
    first[...] = rows
    normed[...] = norm(rows, gain[1:2, :], bias[1:2, :]).astype(jnp.bfloat16)


def mlp_kernel(layer, count, *refs):
    blocks, (w1_own, w1_par, b1_own, b1_par, w2_own, w2_par), outs, rows = (
        refs[:count],
        refs[count : count + 6],
        refs[count + 6 : 2 * count + 6],
        refs[-1],
    )
    for c, n in enumerate(blocks):
        rows[PAD * c : PAD * c + 65, :] = n[...]
    total = None
    for w1, b1, w2 in ((w1_own, b1_own, w2_own), (w1_par, b1_par, w2_par)):
        inner = jnp.dot(rows[...], w1[layer], preferred_element_type=jnp.float32) + b1[layer : layer + 1, :]
        inner = (0.5 * inner * (1.0 + lax.erf(inner * 0.7071067811865476))).astype(jnp.bfloat16)
        part = jnp.dot(inner, w2[layer], preferred_element_type=jnp.float32)
        total = part if total is None else total + part
    for c, y in enumerate(outs):
        y[...] = total[PAD * c : PAD * c + 65].astype(jnp.bfloat16)


def pair_mlp_kernel(n, w1_own, w1_par, b1_own, b1_par, w2_own, w2_par, far, far_par, y, rows):
    rows[0:65, :] = n[...]

    def hidden(w1, b1):
        inner = jnp.dot(rows[...], w1, preferred_element_type=jnp.float32) + b1
        return (0.5 * inner * (1.0 + lax.erf(inner * 0.7071067811865476))).astype(jnp.bfloat16)

    total = None
    for w1, b1, w2 in ((w1_own, b1_own, w2_own), (w1_par, b1_par, w2_par)):
        part = jnp.dot(hidden(w1[1], b1[1:2, :]), w2[1], preferred_element_type=jnp.float32)
        total = part if total is None else total + part
    for w in (far, far_par):
        bias = jnp.sum(w[0, D:HELD, :].astype(jnp.float32), axis=0, keepdims=True)
        inner = hidden(w[0, 0:D, :], bias)
        total += jnp.concatenate(
            [
                jnp.dot(inner, w[1, 512 * j : 512 * j + 512, :], preferred_element_type=jnp.float32)
                for j in range(2)
            ],
            axis=1,
        )
    y[...] = total[:65].astype(jnp.bfloat16)


def last_kernel(idx, first, y0, y1, o_bias, stream, send):
    k = idx[1]
    summed = y0[...].astype(jnp.float32) + y1[...].astype(jnp.float32)
    rows = (first[...] + summed + o_bias[1:2, :]).astype(jnp.bfloat16)
    stream[...] = rows
    send[...] = jnp.where(k == 0, rows[32:64], rows[0:32])


def place_kernel(idx, stream, recv, out):
    k = idx[1]
    out[0, 0:32, :] = jnp.where(k == 0, stream[0:32, :], recv[...])
    out[0, 32:64, :] = jnp.where(k == 0, recv[...], stream[32:64, :])
    out[0, 64:65, :] = stream[64:65, :]


VMEM = pl.BlockSpec(memory_space=pltpu.VMEM)
SMEM = pl.BlockSpec(memory_space=pltpu.SMEM)
HBM = pl.BlockSpec(memory_space=pltpu.HBM)


def block(dtype=jnp.bfloat16, rows=BLOCK):
    return jax.ShapeDtypeStruct((rows, D), dtype)


def call(kernel, args, out_shape, scratch=(), scalars=1, limit=8, out_specs=None, in_specs=None, aliases=None):
    return pl.pallas_call(
        kernel,
        out_shape=out_shape,
        in_specs=in_specs or [SMEM] * scalars + [VMEM] * (len(args) - scalars),
        out_specs=out_specs or ([VMEM] * len(out_shape) if isinstance(out_shape, list) else VMEM),
        scratch_shapes=list(scratch),
        input_output_aliases=aliases or {},
        compiler_params=pltpu.CompilerParams(vmem_limit_bytes=limit << 20),
    )(*args)


def of_layer(layer, array):
    rest = array.shape[1:]
    zeros = (0,) * len(rest)
    return pl.BlockSpec((1, *rest), lambda i: (layer, *zeros))


def shards(
    frames_in,
    frame_time,
    cond_count,
    ln1_gain,
    ln1_bias,
    qkv_weight,
    qkv_bias,
    out_weight,
    out_bias,
    ln2_gain,
    ln2_bias,
    fc1_weight,
    fc1_bias,
    fc2_weight,
    fc2_bias,
):
    part = lax.axis_index("tm")
    pos = lax.axis_index("tensor")
    x, k = pos // 2, pos % 2

    def shift(array, s):
        pairs = [(t, ((t // 2 + s) % NX) * 2 + t % 2) for t in range(2 * NX)]
        return lax.ppermute(array, "tensor", pairs)

    def swap(array):
        return lax.ppermute(array, "tensor", [(t, t ^ 1) for t in range(2 * NX)])

    def spread(array):
        return [array] + [shift(array, -s) for s in (1, 2, 3)]

    def collect(parts):
        return [parts[0]] + [shift(parts[s], s) for s in (1, 2, 3)]

    tie = lax.optimization_barrier
    seen = []

    def attention(layer, message, *late):
        arrived = lax.all_to_all(message, "tm", 0, 0, tiled=True)
        arrived, *late = tie((arrived, *late))
        arrived_par = swap(arrived)
        if layer == 0:
            seen.extend(
                call(
                    tables_kernel,
                    (frame_time, cond_count, *in_hbm(fc1_weight, fc1_bias, fc2_weight)),
                    [
                        jax.ShapeDtypeStruct((FRAMES,), jnp.int32),
                        jax.ShapeDtypeStruct((FRAMES, KEYS), jnp.bfloat16),
                        jax.ShapeDtypeStruct((PARTS, 128), jnp.int32),
                        jax.ShapeDtypeStruct((2, HELD, 512), jnp.bfloat16),
                    ],
                    [pltpu.VMEM((LAYERS, 512), jnp.float32), pltpu.SemaphoreType.DMA((4,))],
                    in_specs=[SMEM] * 2 + [HBM] * 3,
                    out_specs=[SMEM, VMEM, VMEM, VMEM],
                )
            )
        order, mask, row_time, _ = seen
        arrived, arrived_par, *late = tie((arrived, arrived_par, *late))
        late = [swap(a) for a in late]
        mixed = call(
            functools.partial(attn_kernel, layer),
            (idx, order, mask, row_time, arrived, arrived_par),
            jax.ShapeDtypeStruct((PARTS, 24, 128), jnp.bfloat16),
            [
                pltpu.VMEM((256, KEYS), jnp.bfloat16),
                pltpu.VMEM((KEYS, 128), jnp.bfloat16),
                pltpu.VMEM((2, 256, KEYS), jnp.float32),
                pltpu.VMEM((2, 256, KEYS), jnp.bfloat16),
            ],
            scalars=2,
            limit=24,
        )
        mixed, *late = tie((mixed, *late))
        back = lax.all_to_all(mixed, "tm", 0, 0, tiled=True)
        return tie((back, *late))

    message_shape = jax.ShapeDtypeStruct((PARTS, 56, 128), jnp.bfloat16)

    def mlp(layer, blocks):
        outs = {}
        for group in GROUPS:
            done = call(
                functools.partial(mlp_kernel, layer, len(group)),
                (*(blocks[s] for s in group), *(fc1_weight, fc1_par, fc1_bias, fc1_bias_par, fc2_weight, fc2_par)),
                [block()] * len(group),
                [pltpu.VMEM((PAD * len(group), D), jnp.bfloat16)],
                scalars=0,
            )
            outs.update(zip(group, done))
        return [outs[s] for s in range(NX)]

    def in_hbm(*arrays):
        return [pltpu.with_memory_space_constraint(a, pltpu.HBM) for a in arrays]

    biases = jnp.transpose(qkv_bias, (1, 0, 2))
    qkv_par = swap(qkv_weight)
    biases_par = swap(biases)
    fc2_par = swap(fc2_weight)
    idx = jnp.stack([x, k, k == (part // 4) % 2, k == part // 16]).astype(jnp.int32)
    rows, stream, message, held = call(
        start_kernel,
        (idx, *in_hbm(frames_in, qkv_weight, out_weight, biases, ln1_gain, ln1_bias)),
        [
            block(rows=NX * PAD),
            block(),
            message_shape,
            jax.ShapeDtypeStruct((4, HELD, 128), jnp.bfloat16),
        ],
        [
            pltpu.VMEM((8 * BLOCK, D), jnp.bfloat16),
            pltpu.VMEM((8 * BLOCK, D), jnp.float32),
            pltpu.VMEM((3, D, 128), jnp.bfloat16),
            pltpu.VMEM((3, 2, 128), jnp.float32),
            pltpu.VMEM((2, LAYERS, D), jnp.float32),
            pltpu.SemaphoreType.DMA((16,)),
        ],
        in_specs=[SMEM] + [HBM] * 6,
    )
    helds = spread(held)
    held_par = swap(held)
    qkv_par, biases_par, message = tie((qkv_par, biases_par, message))
    message = call(
        partner_kernel,
        (idx, rows, *in_hbm(qkv_par), biases_par, message),
        message_shape,
        [pltpu.VMEM((3, D, 128), jnp.bfloat16), pltpu.SemaphoreType.DMA((3,))],
        in_specs=[SMEM, VMEM, HBM, VMEM, VMEM],
        aliases={4: 0},
    )
    message, fc2_par, held_par, idx, frame_time, cond_count = tie(
        (message, fc2_par, held_par, idx, frame_time, cond_count)
    )
    back, out_par, fc1_par, fc1_bias_par = attention(0, message, out_weight, fc1_weight, fc1_bias)
    partial = pl.pallas_call(
        out_kernel,
        grid=(1,),
        out_shape=[block()] * 4,
        in_specs=[SMEM, VMEM, of_layer(0, out_weight), of_layer(0, out_par)],
        out_specs=[VMEM] * 4,
        scratch_shapes=[pltpu.VMEM((NX * PAD, 128), jnp.bfloat16)] * 2,
        compiler_params=pltpu.CompilerParams(vmem_limit_bytes=12 << 20),
    )(idx, back, out_weight, out_par)
    partial = collect(partial)
    first, normed_two = call(
        functools.partial(mid_kernel, 0),
        (stream, *partial, out_bias, ln2_gain, ln2_bias),
        [block(jnp.float32), block()],
        scalars=0,
    )
    partial = mlp(0, spread(normed_two))
    partial = collect(partial)
    held_pars = [held_par] + [swap(helds[s]) for s in (1, 2, 3)]
    everything = (*in_hbm(*helds), *held_pars)
    stream, message = call(
        turn_kernel,
        (idx, first, *partial, fc2_bias, ln1_gain, ln1_bias, *everything),
        [block(), message_shape],
        [
            pltpu.VMEM((PAD, D), jnp.bfloat16),
            pltpu.VMEM((NX, 3, HELD, 128), jnp.bfloat16),
            pltpu.VMEM((2 * NX, 3, PAD, 128), jnp.float32),
            pltpu.SemaphoreType.DMA((NX,)),
        ],
        in_specs=[SMEM] + [VMEM] * 8 + [HBM] * 4 + [VMEM] * 4,
        limit=14,
    )
    message, packed = tie((message, seen[3]))

    def pair(array, other):
        return lax.ppermute(array, "tensor", [(t, other(t // 2) * 2 + t % 2) for t in range(2 * NX)])

    far = pair(packed, lambda c: c ^ 1)
    (back,) = attention(1, message)
    back, far = tie((back, far))
    far_par = swap(far)
    first, normed_two = call(
        whole_out_kernel,
        (idx, back, stream, out_bias, ln2_gain, ln2_bias, *everything),
        [block(jnp.float32), block()],
        [
            pltpu.VMEM((2 * NX, PAD, 128), jnp.bfloat16),
            pltpu.VMEM((NX, D, 128), jnp.bfloat16),
            pltpu.SemaphoreType.DMA((NX,)),
        ],
        in_specs=[SMEM] + [VMEM] * 5 + [HBM] * 4 + [VMEM] * 4,
    )
    weights = (fc1_weight, fc1_par, fc1_bias, fc1_bias_par, fc2_weight, fc2_par, far, far_par)
    partial = []
    for n in (normed_two, pair(normed_two, lambda c: 3 - c)):
        partial.append(
            call(
                pair_mlp_kernel,
                (n, *weights),
                block(),
                [pltpu.VMEM((PAD, D), jnp.bfloat16)],
                scalars=0,
            )
        )
    added = pair(partial[1], lambda c: 3 - c)
    stream, send = call(
        last_kernel, (idx, first, partial[0], added, fc2_bias), [block(), block(rows=32)]
    )
    recv = swap(send)
    return call(place_kernel, (idx, stream, recv), jax.ShapeDtypeStruct((1, BLOCK, D), jnp.bfloat16))


def solution(mesh):
    in_specs = (
        P("tm", None, None),
        P(),
        P(),
        P(),
        P(),
        P(None, None, None, "tensor"),
        P(None, None, "tensor"),
        P(None, "tensor", None),
        P(),
        P(),
        P(),
        P(None, None, "tensor"),
        P(None, "tensor"),
        P(None, "tensor", None),
        P(),
    )
    out_specs = P("tm", "tensor", None)
    return jax.shard_map(shards, mesh=mesh, in_specs=in_specs, out_specs=out_specs, check_vma=False)
```

```python
import functools

import jax
import jax.numpy as jnp
from jax import lax
from jax.experimental import pallas as pl
from jax.experimental.pallas import tpu as pltpu
from jax.sharding import PartitionSpec as P

D = 1024
LAYERS = 2
PARTS = 32
FRAMES = 16
BLOCK = 65
PAD = 72
KEYS = 2176
NX = 4
HELD = 1032
LOG2E = 1.4426950408889634
SCALE = 0.125 * LOG2E
NEG = -1e30

GROUPS = ((1, 3), (2, 0))


def lanes(shape):
    return lax.broadcasted_iota(jnp.int32, shape, len(shape) - 1)


def subs(shape):
    return lax.broadcasted_iota(jnp.int32, shape, len(shape) - 2)


def norm(rows, gain, bias):
    center = jnp.mean(rows, axis=-1, keepdims=True)
    off = rows - center
    spread = jnp.mean(off * off, axis=-1, keepdims=True)
    return off * lax.rsqrt(spread + 1e-06) * gain + bias


def pack_kernel(w_ref, wo_ref, bias_ref, held, biases, sems):
    copies = [
        pltpu.make_async_copy(w_ref.at[1], held.at[0:3, 0:D, :], sems.at[0]),
        pltpu.make_async_copy(bias_ref, biases, sems.at[1]),
    ]
    for layer in range(LAYERS):
        for j in range(8):
            cols = slice(128 * j, 128 * j + 128)
            copies.append(
                pltpu.make_async_copy(
                    wo_ref.at[layer, :, cols], held.at[4 - layer, cols, :], sems.at[2 + 8 * layer + j]
                )
            )
    for copy in copies:
        copy.start()
    for copy in copies:
        copy.wait()
    for i in range(3):
        held[i, D:HELD, :] = split_rows(biases[i, 1:2, :])
    for i in (3, 4):
        held[i, D:HELD, :] = jnp.zeros((8, 128), jnp.bfloat16)


def tables_kernel(frame_time, cond_count, order, mask, row_time):
    for f in range(FRAMES):
        order[frame_time[f]] = f
    slot_time = jnp.full((FRAMES, 128), FRAMES, jnp.int32)
    times = jnp.zeros((PARTS, 128), jnp.int32)
    for g in range(PARTS):
        time = frame_time[g // 2]
        seen = jnp.where(g % 2 < cond_count[g // 2], time, FRAMES)
        slot_time = jnp.where(lanes(slot_time.shape) == g, seen, slot_time)
        times = jnp.where(subs(times.shape) == g, time, times)
    row_time[...] = times
    mask[:, 0:128] = jnp.where(slot_time <= subs(slot_time.shape), 0.0, NEG).astype(jnp.bfloat16)
    for t in range(FRAMES):
        seen = jnp.where(subs((FRAMES, 128)) >= t, 0.0, NEG)
        mask[:, 128 * t + 128 : 128 * t + 256] = seen.astype(jnp.bfloat16)


def load_kernel(planes, *refs):
    held, (out, sems) = refs[:5], refs[5:]
    copies = [pltpu.make_async_copy(ref.at[planes], out.at[c], sems.at[c]) for c, ref in enumerate(held)]
    for copy in copies:
        copy.start()
    for copy in copies:
        copy.wait()


def load_far_kernel(h0, h1, h2, h3, h4, w1_ref, b1_ref, w2_ref, out, packed, bias, sems):
    copies = [
        pltpu.make_async_copy(ref.at[4:5], out.at[c], sems.at[4 + c])
        for c, ref in enumerate((h0, h1, h2, h3, h4))
    ]
    copies += [
        pltpu.make_async_copy(w1_ref.at[1], packed.at[0, 0:D], sems.at[0]),
        pltpu.make_async_copy(w2_ref.at[1, :, 0:512], packed.at[1, 0:512], sems.at[1]),
        pltpu.make_async_copy(w2_ref.at[1, :, 512:D], packed.at[1, 512:D], sems.at[2]),
        pltpu.make_async_copy(b1_ref, bias, sems.at[3]),
    ]
    for copy in copies:
        copy.start()
    for copy in copies:
        copy.wait()
    packed[0, D:HELD, :] = split_rows(bias[1:2, :])
    packed[1, D:HELD, :] = jnp.zeros((8, 512), jnp.bfloat16)


def split_rows(row):
    high = row.astype(jnp.bfloat16).astype(jnp.float32)
    middle = (row - high).astype(jnp.bfloat16).astype(jnp.float32)
    lowest = (row - high) - middle
    sub = subs((8, row.shape[1]))
    rows = jnp.where(sub == 0, high, jnp.where(sub == 1, middle, jnp.where(sub == 2, lowest, 0.0)))
    return rows.astype(jnp.bfloat16)


def from_row(ref, base, off, count):
    return pltpu.roll(ref[pl.ds(pl.multiple_of(base, 8), count), :], lax.rem(count - off, count), 0)


def emit(out, q, key, val, places, tails):
    low = lanes(q.shape) < 64
    low8 = lanes((8, 128)) < 64
    sub = lax.broadcasted_iota(jnp.int32, (8, 128), 0)
    q_r, key_r, val_r = (pltpu.roll(a, 64, 1) for a in (q, key, val))
    for hl in range(2):
        if hl == 0:
            kv = jnp.where(low, key, val_r)
            q_lo, q_hi = q, q_r
        else:
            kv = jnp.where(low, key_r, val)
            q_lo, q_hi = q_r, q
        for slot, at in places:
            out[slot + hl, 0:32, :] = kv[at : at + 32].astype(jnp.bfloat16)
            out[slot + hl, 32:48, :] = jnp.where(
                low[:16], q_lo[at : at + 16], q_hi[at + 16 : at + 32]
            ).astype(jnp.bfloat16)
            out[slot + hl, 48:56, :] = jnp.zeros((8, 128), jnp.bfloat16)
        for slot, at in tails:
            tail = jnp.where(
                sub == 0,
                jnp.broadcast_to(kv[at : at + 1], (8, 128)),
                jnp.where((sub == 1) & low8, jnp.broadcast_to(q_lo[at : at + 1], (8, 128)), 0.0),
            )
            out[slot + hl, 48:56, :] = tail.astype(jnp.bfloat16)


def start_kernel(
    idx, x_ref, w_own, w_par, b_own, b_par, g_ref, b_ref, xrows, out, raw, wide, rows, w, biases, norms, sems
):
    x, k = idx[0], idx[1]
    first = [
        pltpu.make_async_copy(x_ref.at[0], raw, sems.at[0]),
        pltpu.make_async_copy(g_ref, norms.at[0], sems.at[1]),
        pltpu.make_async_copy(b_ref, norms.at[1], sems.at[2]),
        pltpu.make_async_copy(b_own, biases, sems.at[3]),
    ]
    weights = [pltpu.make_async_copy(ref.at[0], w.at[c], sems.at[4 + c]) for c, ref in enumerate((w_own, w_par))]
    for copy in first + weights:
        copy.start()
    for copy in first:
        copy.wait()
    wide[...] = raw[...].astype(jnp.float32)
    gain, bias = norms[0, 0:1, :], norms[1, 0:1, :]
    for s in range(NX):
        chip = lax.rem(x + s, NX)
        for b in range(2):
            part = from_row(wide, 64 * (2 * chip + b) + 32 * k, 2 * chip + b, 40)[:32]
            at = PAD * s + 32 * b
            rows[at : at + 32, :] = norm(part, gain, bias).astype(jnp.bfloat16)
            xrows[at : at + 32, :] = part.astype(jnp.bfloat16)
        part = from_row(wide, 64 * (2 * chip + k) + 64, 2 * chip + k, 8)
        at = PAD * s + 64
        rows[at : at + 8, :] = norm(part, gain, bias).astype(jnp.bfloat16)
        xrows[at : at + 8, :] = part.astype(jnp.bfloat16)
    for copy in weights:
        copy.wait()
    both = jnp.concatenate([w[c, i] for c in range(2) for i in range(3)], axis=1)
    both = jnp.dot(rows[...], both, preferred_element_type=jnp.float32)
    for c, (side, row) in enumerate(((k, biases), (1 - k, b_par))):
        places = [(s * 8 + b * 4 + 2 * side, PAD * s + 32 * b) for s in range(NX) for b in range(2)]
        tails = [(s * 8 + k * 4 + 2 * side, PAD * s + 64) for s in range(NX)]
        parts = [both[:, 384 * c + 128 * i : 384 * c + 128 * i + 128] + row[i, 0:1, :] for i in range(3)]
        emit(out, *parts, places, tails)


def turn_kernel(idx, first, y0, y1, y2, y3, o_bias, gain, bias, *rest):
    w, *near, stream, out, rows, acc = rest
    k = idx[1]
    summed = (y0[...].astype(jnp.float32) + y1[...].astype(jnp.float32)) + (
        y2[...].astype(jnp.float32) + y3[...].astype(jnp.float32)
    )
    new = (first[...] + summed + o_bias[0:1, :]).astype(jnp.bfloat16)
    stream[...] = new
    rows[0:65, :] = norm(new.astype(jnp.float32), gain[1:2, :], bias[1:2, :]).astype(jnp.bfloat16)

    def project(slots, refs):
        weight = jnp.concatenate([ref[i, 0:D, :] for ref in refs for i in range(3)], axis=1)
        total = jnp.dot(rows[...], weight, preferred_element_type=jnp.float32)
        for c, (slot, ref) in enumerate(zip(slots, refs)):
            for i in range(3):
                row = jnp.sum(ref[i, D:HELD, :].astype(jnp.float32), axis=0, keepdims=True)
                at = 384 * c + 128 * i
                acc[slot, i] = total[:, at : at + 128] + row

    project((3, 5), near[0:2])
    project((7, 1), (near[2], w.at[4]))
    project((0, 2), (w.at[0], w.at[1]))
    project((4, 6), (w.at[2], w.at[3]))

    def one(c, carry):
        base = c // 2 * 4 + 2 * lax.rem(k + c, 2)
        emit(out, acc[c, 0], acc[c, 1], acc[c, 2], [(base, 0), (16 + base, 32)], [(k * 16 + base, 64)])
        return carry

    lax.fori_loop(0, 2 * NX, one, 0)


def attn_kernel(layer, idx, order, mask, part_time, r_own, r_par, out, kt, vals, score, prob):
    mine = idx[2 + layer]
    low = lanes((128, 128)) < 64

    def place(at, block):
        key, val = block.astype(jnp.float32), block
        both = jnp.where(low, key, pltpu.roll(key, 64, 1))
        kt[0:128, at : at + 128] = both.T.astype(jnp.bfloat16)
        vals[at : at + 128, :] = jnp.where(low, jnp.ones_like(val), val)

    def queries(packed, which):
        scaled = packed * SCALE
        high = scaled.astype(jnp.bfloat16).astype(jnp.float32)
        rest = scaled - high
        left = jnp.where(lanes(packed.shape) < 64, high, pltpu.roll(rest, 64, 1))
        return jnp.concatenate([left.astype(jnp.bfloat16), which.astype(jnp.bfloat16)], axis=1)

    sub = lax.broadcasted_iota(jnp.int32, (PARTS, 8, 128), 1)
    tail_own = r_own[:, 48:56, :].astype(jnp.float32)
    tail_par = r_par[:, 48:56, :].astype(jnp.float32)
    extra = jnp.sum(jnp.where(sub == 0, jnp.where(mine == 1, tail_own, tail_par), 0.0), axis=1)
    place(0, jnp.concatenate([extra, jnp.zeros((96, 128), jnp.float32)], axis=0).astype(jnp.bfloat16))
    kt[128:144, :] = mask[...]
    kt[144:256, :] = jnp.zeros((112, KEYS), jnp.bfloat16)
    for t in range(FRAMES):
        at = pl.ds(2 * order[t], 2)
        own = r_own[at, 0:32, :].reshape(64, 128)
        par = r_par[at, 0:32, :].reshape(64, 128)
        place(128 * t + 128, jnp.concatenate([own, par], axis=0))

    def attend(lhs, rows, n, buf):
        score[buf, 0:rows, 0:n] = jnp.dot(lhs, kt[:, 0:n], preferred_element_type=jnp.float32)
        for r in range(0, rows, 16):
            now = score[buf, r : r + 16, 0:n]
            now = jnp.exp2(now - jnp.max(now, axis=1, keepdims=True))
            prob[buf, r : r + 16, 0:n] = now.astype(jnp.bfloat16)
        mixed = jnp.dot(prob[buf, 0:rows, 0:n], vals[0:n, :], preferred_element_type=jnp.float32)
        return mixed / pltpu.roll(mixed, 64, 1)

    row = lax.broadcasted_iota(jnp.int32, (256, 128), 0)
    for i in range(4):
        packed = jnp.concatenate(
            [r_own[pl.ds(2 * order[4 * i + t], 2), 32:48, :].reshape(32, 128) for t in range(4)], axis=0
        ).astype(jnp.float32)
        packed = jnp.concatenate([packed, pltpu.roll(packed, 64, 1)], axis=0)
        which = jnp.where(lanes((256, 128)) == 4 * i + (row % 128) // 32, 1.0, 0.0)
        res = attend(queries(packed, which), 256, 128 + 512 * (i + 1), i % 2)
        merged = jnp.where(low, pltpu.roll(res[:128], 64, 1), res[128:]).astype(jnp.bfloat16)
        for t in range(4):
            out[pl.ds(2 * order[4 * i + t], 2), 0:16, :] = merged[32 * t : 32 * t + 32].reshape(2, 16, 128)
    packed = jnp.sum(jnp.where(sub == 1, tail_own, 0.0), axis=1)
    which = jnp.where(lanes((PARTS, 128)) == part_time[...], 1.0, 0.0)
    res = pltpu.roll(attend(queries(packed, which), PARTS, KEYS, 0), 64, 1)
    out[:, 16:24, :] = jnp.broadcast_to(res[:, None, :], (PARTS, 8, 128)).astype(jnp.bfloat16)


def pair(first, second):
    low = lanes((24, 128)) < 64
    first, second = first.astype(jnp.float32), second.astype(jnp.float32)
    return (
        jnp.where(low, first, pltpu.roll(second, 64, 1)).astype(jnp.bfloat16),
        jnp.where(low, pltpu.roll(first, 64, 1), second).astype(jnp.bfloat16),
    )


def gather_heads(dst, at, back, patches, tail):
    for b, slot in enumerate(patches):
        lo, hi = pair(back[slot], back[slot + 1])
        dst[at + 32 * b : at + 32 * b + 16, :] = lo[:16]
        dst[at + 32 * b + 16 : at + 32 * b + 32, :] = hi[:16]
    lo, _ = pair(back[tail], back[tail + 1])
    dst[at + 64 : at + 72, :] = lo[16:24]


def heads_kernel(idx, back, out):
    k = idx[1]
    for c, side in enumerate((k, 1 - k)):
        for s in range(NX):
            slots = [s * 8 + b * 4 + 2 * side for b in range(2)]
            cols = slice(128 * c, 128 * c + 128)
            gather_heads(out.at[:, cols], PAD * s, back, slots, s * 8 + k * 4 + 2 * side)


def blocks_of(plane):
    return jnp.concatenate([plane[128 * j : 128 * j + 128, :] for j in range(8)], axis=1)


def every_out_kernel(h0, h1, h2, h3, xrows, o_bias, gain, bias, *rest):
    w, *near, first, normed, lhs = rest
    for s, heads in enumerate((h0, h1, h2, h3)):
        for r in range(NX):
            at = PAD * ((r - s) % NX)
            lhs[PAD * r : PAD * r + PAD, 256 * s : 256 * s + 256] = heads[at : at + PAD, :]
    weight = jnp.concatenate(
        [blocks_of(p) for s in range(NX) for p in (w.at[s, 0], near[s - 1].at[4] if s else w.at[4, 0])], axis=0
    )
    total = jnp.dot(lhs[...], weight, preferred_element_type=jnp.float32)
    rows = xrows[...].astype(jnp.float32) + total + o_bias[0:1, :]
    first[...] = rows[0:65]
    normed[...] = norm(rows, gain[0:1, :], bias[0:1, :]).astype(jnp.bfloat16)


def whole_out_kernel(idx, back, own, o_bias, gain, bias, *rest):
    w, *near, first, normed, heads = rest
    k = idx[1]
    for s in range(NX):
        for c, side in enumerate((k, 1 - k)):
            base = s * 4 + 2 * side
            at = 256 * s + 128 * c
            gather_heads(heads.at[:, at : at + 128], 0, back, [base, 16 + base], k * 16 + base)
    weight = jnp.concatenate(
        [blocks_of(p) for s in range(NX) for p in (w.at[s, 0], near[s - 1].at[3] if s else w.at[4, 0])], axis=0
    )
    total = jnp.dot(heads[...], weight, preferred_element_type=jnp.float32)
    rows = own[...].astype(jnp.float32) + total[:65] + o_bias[1:2, :]
    first[...] = rows
    normed[...] = norm(rows, gain[1:2, :], bias[1:2, :]).astype(jnp.bfloat16)


def mlp_kernel(group, n, w1_own, w1_par, b1_own, b1_par, w2_own, w2_par, *rest):
    outs, rows = rest[:-1], rest[-1]
    for c, s in enumerate(group):
        rows[PAD * c : PAD * c + PAD, :] = n[PAD * s : PAD * s + PAD, :]
    total = None
    for w1, b1, w2 in ((w1_own, b1_own, w2_own), (w1_par, b1_par, w2_par)):
        inner = jnp.dot(rows[...], w1[0], preferred_element_type=jnp.float32) + b1[0:1, :]
        inner = (0.5 * inner * (1.0 + lax.erf(inner * 0.7071067811865476))).astype(jnp.bfloat16)
        part = jnp.dot(inner, w2[0], preferred_element_type=jnp.float32)
        total = part if total is None else total + part
    for c, y in enumerate(outs):
        y[...] = total[PAD * c : PAD * c + 65].astype(jnp.bfloat16)


def pair_mlp_kernel(n, w1_own, w1_par, b1_own, b1_par, w2_own, w2_par, far, far_par, y, rows):
    rows[0:65, :] = n[...]

    def hidden(w1, b1):
        inner = jnp.dot(rows[...], w1, preferred_element_type=jnp.float32) + b1
        return (0.5 * inner * (1.0 + lax.erf(inner * 0.7071067811865476))).astype(jnp.bfloat16)

    total = None
    for w1, b1, w2 in ((w1_own, b1_own, w2_own), (w1_par, b1_par, w2_par)):
        part = jnp.dot(hidden(w1[1], b1[1:2, :]), w2[1], preferred_element_type=jnp.float32)
        total = part if total is None else total + part
    for w in (far, far_par):
        bias = jnp.sum(w[0, D:HELD, :].astype(jnp.float32), axis=0, keepdims=True)
        inner = hidden(w[0, 0:D, :], bias)
        total += jnp.concatenate(
            [
                jnp.dot(inner, w[1, 512 * j : 512 * j + 512, :], preferred_element_type=jnp.float32)
                for j in range(2)
            ],
            axis=1,
        )
    y[...] = total[:65].astype(jnp.bfloat16)


def last_kernel(idx, first, y0, y1, o_bias, stream, send):
    k = idx[1]
    summed = y0[...].astype(jnp.float32) + y1[...].astype(jnp.float32)
    rows = (first[...] + summed + o_bias[1:2, :]).astype(jnp.bfloat16)
    stream[...] = rows
    send[...] = jnp.where(k == 0, rows[32:64], rows[0:32])


def place_kernel(idx, stream, recv, out):
    k = idx[1]
    out[0, 0:32, :] = jnp.where(k == 0, stream[0:32, :], recv[...])
    out[0, 32:64, :] = jnp.where(k == 0, recv[...], stream[32:64, :])
    out[0, 64:65, :] = stream[64:65, :]


VMEM = pl.BlockSpec(memory_space=pltpu.VMEM)
SMEM = pl.BlockSpec(memory_space=pltpu.SMEM)
HBM = pl.BlockSpec(memory_space=pltpu.HBM)


def block(dtype=jnp.bfloat16, rows=BLOCK):
    return jax.ShapeDtypeStruct((rows, D), dtype)


def call(kernel, args, out_shape, scratch=(), scalars=1, limit=8, out_specs=None, in_specs=None, aliases=None):
    return pl.pallas_call(
        kernel,
        out_shape=out_shape,
        in_specs=in_specs or [SMEM] * scalars + [VMEM] * (len(args) - scalars),
        out_specs=out_specs or ([VMEM] * len(out_shape) if isinstance(out_shape, list) else VMEM),
        scratch_shapes=list(scratch),
        input_output_aliases=aliases or {},
        compiler_params=pltpu.CompilerParams(vmem_limit_bytes=limit << 20),
    )(*args)


def shards(
    frames_in,
    frame_time,
    cond_count,
    ln1_gain,
    ln1_bias,
    qkv_weight,
    qkv_bias,
    out_weight,
    out_bias,
    ln2_gain,
    ln2_bias,
    fc1_weight,
    fc1_bias,
    fc2_weight,
    fc2_bias,
):
    part = lax.axis_index("tm")
    pos = lax.axis_index("tensor")
    x, k = pos // 2, pos % 2

    def shift(array, s):
        pairs = [(t, ((t // 2 + s) % NX) * 2 + t % 2) for t in range(2 * NX)]
        return lax.ppermute(array, "tensor", pairs)

    def swap(array):
        return lax.ppermute(array, "tensor", [(t, t ^ 1) for t in range(2 * NX)])

    def spread(array):
        return [array] + [shift(array, -s) for s in (1, 2, 3)]

    def collect(parts):
        return [parts[0]] + [shift(parts[s], s) for s in (1, 2, 3)]

    tie = lax.optimization_barrier

    seen = []

    def attention(layer, message, beside, *late):
        arrived = lax.all_to_all(message, "tm", 0, 0, tiled=True)
        arrived, *late = tie((arrived, *late))
        arrived_par = swap(arrived)
        seen.append(beside())
        order, mask, row_time = seen[0]
        arrived, arrived_par, *late = tie((arrived, arrived_par, *late))
        late = [swap(a) for a in late]
        mixed = call(
            functools.partial(attn_kernel, layer),
            (idx, order, mask, row_time, arrived, arrived_par),
            jax.ShapeDtypeStruct((PARTS, 24, 128), jnp.bfloat16),
            [
                pltpu.VMEM((256, KEYS), jnp.bfloat16),
                pltpu.VMEM((KEYS, 128), jnp.bfloat16),
                pltpu.VMEM((2, 256, KEYS), jnp.float32),
                pltpu.VMEM((2, 256, KEYS), jnp.bfloat16),
            ],
            scalars=2,
            limit=24,
        )
        mixed, *late = tie((mixed, *late))
        back = lax.all_to_all(mixed, "tm", 0, 0, tiled=True)
        return tie((back, *late))

    message_shape = jax.ShapeDtypeStruct((PARTS, 56, 128), jnp.bfloat16)

    def in_hbm(*arrays):
        return [pltpu.with_memory_space_constraint(a, pltpu.HBM) for a in arrays]

    biases = jnp.transpose(qkv_bias, (1, 0, 2))
    qkv_par = swap(qkv_weight)
    biases_par = swap(biases)
    fc2_par = swap(fc2_weight)
    idx = jnp.stack([x, k, k == (part // 4) % 2, k == part // 16]).astype(jnp.int32)
    held = call(
        pack_kernel,
        in_hbm(qkv_weight, out_weight, biases),
        jax.ShapeDtypeStruct((5, HELD, 128), jnp.bfloat16),
        [pltpu.VMEM((3, LAYERS, 128), jnp.float32), pltpu.SemaphoreType.DMA((18,))],
        in_specs=[HBM] * 3,
    )
    helds = spread(held)
    held_par = swap(held)
    xrows, message = call(
        start_kernel,
        (idx, *in_hbm(frames_in, qkv_weight, qkv_par, biases), biases_par, *in_hbm(ln1_gain, ln1_bias)),
        [block(rows=NX * PAD), message_shape],
        [
            pltpu.VMEM((8 * BLOCK, D), jnp.bfloat16),
            pltpu.VMEM((8 * BLOCK, D), jnp.float32),
            pltpu.VMEM((NX * PAD, D), jnp.bfloat16),
            pltpu.VMEM((2, 3, D, 128), jnp.bfloat16),
            pltpu.VMEM((3, LAYERS, 128), jnp.float32),
            pltpu.VMEM((2, LAYERS, D), jnp.float32),
            pltpu.SemaphoreType.DMA((6,)),
        ],
        in_specs=[SMEM, HBM, HBM, HBM, HBM, VMEM, HBM, HBM],
        limit=12,
    )
    message, fc2_par, held_par = tie((message, fc2_par, held_par))

    def tables():
        return call(
            tables_kernel,
            (frame_time, cond_count),
            [
                jax.ShapeDtypeStruct((FRAMES,), jnp.int32),
                jax.ShapeDtypeStruct((FRAMES, KEYS), jnp.bfloat16),
                jax.ShapeDtypeStruct((PARTS, 128), jnp.int32),
            ],
            scalars=2,
            out_specs=[SMEM, VMEM, VMEM],
        )

    def load(planes, count, rows):
        return call(
            functools.partial(load_kernel, planes),
            far_refs,
            jax.ShapeDtypeStruct((5, count, rows, 128), jnp.bfloat16),
            [pltpu.SemaphoreType.DMA((5,))],
            in_specs=[HBM] * 5,
        )

    back, fc1_par, fc1_bias_par = attention(0, message, tables, fc1_weight, fc1_bias)
    heads = call(heads_kernel, (idx, back), jax.ShapeDtypeStruct((NX * PAD, 256), jnp.bfloat16))
    heads = spread(heads)
    held_pars = [held_par] + [swap(helds[s]) for s in (1, 2, 3)]
    far_refs = in_hbm(*helds, held_pars[0])
    near = held_pars[1:]
    loaded, packed = call(
        load_far_kernel,
        (*far_refs, *in_hbm(fc1_weight, fc1_bias, fc2_weight)),
        [jax.ShapeDtypeStruct((5, 1, HELD, 128), jnp.bfloat16), jax.ShapeDtypeStruct((2, HELD, 512), jnp.bfloat16)],
        [pltpu.VMEM((LAYERS, 512), jnp.float32), pltpu.SemaphoreType.DMA((9,))],
        in_specs=[HBM] * 8,
    )
    first, normed_two = call(
        every_out_kernel,
        (*heads, xrows, out_bias, ln2_gain, ln2_bias, loaded, *near),
        [block(jnp.float32), block(rows=NX * PAD)],
        [pltpu.VMEM((NX * PAD, D), jnp.bfloat16)],
        scalars=0,
    )
    partial = {}
    for group in GROUPS:
        done = call(
            functools.partial(mlp_kernel, group),
            (normed_two, fc1_weight, fc1_par, fc1_bias, fc1_bias_par, fc2_weight, fc2_par),
            [block()] * len(group),
            [pltpu.VMEM((PAD * len(group), D), jnp.bfloat16)],
            scalars=0,
        )
        partial.update(zip(group, done))
    loaded = load(slice(0, 3), 3, HELD)
    partial = collect(partial)
    stream, message = call(
        turn_kernel,
        (idx, first, *partial, fc2_bias, ln1_gain, ln1_bias, loaded, *near),
        [block(), message_shape],
        [pltpu.VMEM((PAD, D), jnp.bfloat16), pltpu.VMEM((2 * NX, 3, PAD, 128), jnp.float32)],
    )
    message, packed = tie((message, packed))

    def pair(array, other):
        return lax.ppermute(array, "tensor", [(t, other(t // 2) * 2 + t % 2) for t in range(2 * NX)])

    far = pair(packed, lambda c: c ^ 1)
    (back,) = attention(1, message, lambda: load(slice(3, 4), 1, HELD))
    back, far, loaded = tie((back, far, seen[1]))
    far_par = swap(far)
    first, normed_two = call(
        whole_out_kernel,
        (idx, back, stream, out_bias, ln2_gain, ln2_bias, loaded, *near),
        [block(jnp.float32), block()],
        [pltpu.VMEM((PAD, D), jnp.bfloat16)],
    )
    weights = (fc1_weight, fc1_par, fc1_bias, fc1_bias_par, fc2_weight, fc2_par, far, far_par)
    partial = []
    for n in (normed_two, pair(normed_two, lambda c: 3 - c)):
        partial.append(
            call(
                pair_mlp_kernel,
                (n, *weights),
                block(),
                [pltpu.VMEM((PAD, D), jnp.bfloat16)],
                scalars=0,
            )
        )
    added = pair(partial[1], lambda c: 3 - c)
    stream, send = call(
        last_kernel, (idx, first, partial[0], added, fc2_bias), [block(), block(rows=32)]
    )
    recv = swap(send)
    return call(place_kernel, (idx, stream, recv), jax.ShapeDtypeStruct((1, BLOCK, D), jnp.bfloat16))


def solution(mesh):
    in_specs = (
        P("tm", None, None),
        P(),
        P(),
        P(),
        P(),
        P(None, None, None, "tensor"),
        P(None, None, "tensor"),
        P(None, "tensor", None),
        P(),
        P(),
        P(),
        P(None, None, "tensor"),
        P(None, "tensor"),
        P(None, "tensor", None),
        P(),
    )
    out_specs = P("tm", "tensor", None)
    return jax.shard_map(shards, mesh=mesh, in_specs=in_specs, out_specs=out_specs, check_vma=False)
```

```python
import functools

import jax
import jax.numpy as jnp
from jax import lax
from jax.experimental import pallas as pl
from jax.experimental.pallas import tpu as pltpu
from jax.sharding import PartitionSpec as P

D = 1024
LAYERS = 2
PARTS = 32
FRAMES = 16
BLOCK = 65
PAD = 72
KEYS = 2176
NX = 4
HELD = 1032
LOG2E = 1.4426950408889634
SCALE = 0.125 * LOG2E
NEG = -1e30

GROUPS = ((1, 3, 2, 0),)


def lanes(shape):
    return lax.broadcasted_iota(jnp.int32, shape, len(shape) - 1)


def subs(shape):
    return lax.broadcasted_iota(jnp.int32, shape, len(shape) - 2)


def norm(rows, gain, bias):
    center = jnp.mean(rows, axis=-1, keepdims=True)
    off = rows - center
    spread = jnp.mean(off * off, axis=-1, keepdims=True)
    return off * lax.rsqrt(spread + 1e-06) * gain + bias


def pack_kernel(w_ref, wo_ref, bias_ref, held, biases, sems):
    copies = [
        pltpu.make_async_copy(w_ref.at[1], held.at[0:3, 0:D, :], sems.at[0]),
        pltpu.make_async_copy(bias_ref, biases, sems.at[1]),
    ]
    for layer in range(LAYERS):
        for j in range(8):
            cols = slice(128 * j, 128 * j + 128)
            copies.append(
                pltpu.make_async_copy(
                    wo_ref.at[layer, :, cols], held.at[4 - layer, cols, :], sems.at[2 + 8 * layer + j]
                )
            )
    for copy in copies:
        copy.start()
    for copy in copies:
        copy.wait()
    for i in range(3):
        held[i, D:HELD, :] = split_rows(biases[i, 1:2, :])
    for i in (3, 4):
        held[i, D:HELD, :] = jnp.zeros((8, 128), jnp.bfloat16)


def tables_kernel(frame_time, cond_count, order, mask, row_time):
    for f in range(FRAMES):
        order[frame_time[f]] = f
    slot_time = jnp.full((FRAMES, 128), FRAMES, jnp.int32)
    times = jnp.zeros((PARTS, 128), jnp.int32)
    for g in range(PARTS):
        time = frame_time[g // 2]
        seen = jnp.where(g % 2 < cond_count[g // 2], time, FRAMES)
        slot_time = jnp.where(lanes(slot_time.shape) == g, seen, slot_time)
        times = jnp.where(subs(times.shape) == g, time, times)
    row_time[...] = times
    mask[:, 0:128] = jnp.where(slot_time <= subs(slot_time.shape), 0.0, NEG).astype(jnp.bfloat16)
    for t in range(FRAMES):
        seen = jnp.where(subs((FRAMES, 128)) >= t, 0.0, NEG)
        mask[:, 128 * t + 128 : 128 * t + 256] = seen.astype(jnp.bfloat16)


def load_kernel(planes, *refs):
    *held, out, sems = refs
    copies = [pltpu.make_async_copy(ref.at[planes], out.at[c], sems.at[c]) for c, ref in enumerate(held)]
    for copy in copies:
        copy.start()
    for copy in copies:
        copy.wait()


def load_mlp_kernel(w1_ref, b1_ref, w2_ref, packed, w1, w2, bias, sems):
    copies = [
        pltpu.make_async_copy(w1_ref.at[0], w1, sems.at[4]),
        pltpu.make_async_copy(w2_ref.at[0], w2, sems.at[5]),
        pltpu.make_async_copy(w1_ref.at[1], packed.at[0, 0:D], sems.at[0]),
        pltpu.make_async_copy(w2_ref.at[1, :, 0:512], packed.at[1, 0:512], sems.at[1]),
        pltpu.make_async_copy(w2_ref.at[1, :, 512:D], packed.at[1, 512:D], sems.at[2]),
        pltpu.make_async_copy(b1_ref, bias, sems.at[3]),
    ]
    for copy in copies:
        copy.start()
    for copy in copies:
        copy.wait()
    packed[0, D:HELD, :] = split_rows(bias[1:2, :])
    packed[1, D:HELD, :] = jnp.zeros((8, 512), jnp.bfloat16)


def split_rows(row):
    high = row.astype(jnp.bfloat16).astype(jnp.float32)
    middle = (row - high).astype(jnp.bfloat16).astype(jnp.float32)
    lowest = (row - high) - middle
    sub = subs((8, row.shape[1]))
    rows = jnp.where(sub == 0, high, jnp.where(sub == 1, middle, jnp.where(sub == 2, lowest, 0.0)))
    return rows.astype(jnp.bfloat16)


def from_row(ref, base, off, count):
    return pltpu.roll(ref[pl.ds(pl.multiple_of(base, 8), count), :], lax.rem(count - off, count), 0)


def emit(out, q, key, val, places, tails):
    low = lanes(q.shape) < 64
    low8 = lanes((8, 128)) < 64
    sub = lax.broadcasted_iota(jnp.int32, (8, 128), 0)
    q_r, key_r, val_r = (pltpu.roll(a, 64, 1) for a in (q, key, val))
    for hl in range(2):
        if hl == 0:
            kv = jnp.where(low, key, val_r)
            q_lo, q_hi = q, q_r
        else:
            kv = jnp.where(low, key_r, val)
            q_lo, q_hi = q_r, q
        for slot, at in places:
            out[slot + hl, 0:32, :] = kv[at : at + 32].astype(jnp.bfloat16)
            out[slot + hl, 32:48, :] = jnp.where(
                low[:16], q_lo[at : at + 16], q_hi[at + 16 : at + 32]
            ).astype(jnp.bfloat16)
            out[slot + hl, 48:56, :] = jnp.zeros((8, 128), jnp.bfloat16)
        for slot, at in tails:
            tail = jnp.where(
                sub == 0,
                jnp.broadcast_to(kv[at : at + 1], (8, 128)),
                jnp.where((sub == 1) & low8, jnp.broadcast_to(q_lo[at : at + 1], (8, 128)), 0.0),
            )
            out[slot + hl, 48:56, :] = tail.astype(jnp.bfloat16)


def start_kernel(
    idx, x_ref, w_own, w_par, b_own, b_par, g_ref, b_ref, xrows, out, raw, wide, rows, w, biases, norms, sems
):
    x, k = idx[0], idx[1]
    first = [
        pltpu.make_async_copy(x_ref.at[0], raw, sems.at[0]),
        pltpu.make_async_copy(g_ref, norms.at[0], sems.at[1]),
        pltpu.make_async_copy(b_ref, norms.at[1], sems.at[2]),
        pltpu.make_async_copy(b_own, biases, sems.at[3]),
    ]
    weights = [pltpu.make_async_copy(ref.at[0], w.at[c], sems.at[4 + c]) for c, ref in enumerate((w_own, w_par))]
    for copy in first + weights:
        copy.start()
    for copy in first:
        copy.wait()
    wide[...] = raw[...].astype(jnp.float32)
    gain, bias = norms[0, 0:1, :], norms[1, 0:1, :]
    for s in range(NX):
        chip = lax.rem(x + s, NX)
        for b in range(2):
            part = from_row(wide, 64 * (2 * chip + b) + 32 * k, 2 * chip + b, 40)[:32]
            at = PAD * s + 32 * b
            rows[at : at + 32, :] = norm(part, gain, bias).astype(jnp.bfloat16)
            xrows[at : at + 32, :] = part.astype(jnp.bfloat16)
        part = from_row(wide, 64 * (2 * chip + k) + 64, 2 * chip + k, 8)
        at = PAD * s + 64
        rows[at : at + 8, :] = norm(part, gain, bias).astype(jnp.bfloat16)
        xrows[at : at + 8, :] = part.astype(jnp.bfloat16)
    for copy in weights:
        copy.wait()
    both = jnp.concatenate([w[c, i] for c in range(2) for i in range(3)], axis=1)
    both = jnp.dot(rows[...], both, preferred_element_type=jnp.float32)
    for c, (side, row) in enumerate(((k, biases), (1 - k, b_par))):
        places = [(s * 8 + b * 4 + 2 * side, PAD * s + 32 * b) for s in range(NX) for b in range(2)]
        tails = [(s * 8 + k * 4 + 2 * side, PAD * s + 64) for s in range(NX)]
        parts = [both[:, 384 * c + 128 * i : 384 * c + 128 * i + 128] + row[i, 0:1, :] for i in range(3)]
        emit(out, *parts, places, tails)


def turn_kernel(idx, first, y0, y1, y2, y3, o_bias, gain, bias, *rest):
    w, *near, stream, out, rows, acc = rest
    k = idx[1]
    summed = (y0[...].astype(jnp.float32) + y1[...].astype(jnp.float32)) + (
        y2[...].astype(jnp.float32) + y3[...].astype(jnp.float32)
    )
    new = (first[...] + summed + o_bias[0:1, :]).astype(jnp.bfloat16)
    stream[...] = new
    rows[0:65, :] = norm(new.astype(jnp.float32), gain[1:2, :], bias[1:2, :]).astype(jnp.bfloat16)

    def project(slots, refs):
        weight = jnp.concatenate([ref[i, 0:D, :] for ref in refs for i in range(3)], axis=1)
        total = jnp.dot(rows[...], weight, preferred_element_type=jnp.float32)
        for c, (slot, ref) in enumerate(zip(slots, refs)):
            for i in range(3):
                row = jnp.sum(ref[i, D:HELD, :].astype(jnp.float32), axis=0, keepdims=True)
                at = 384 * c + 128 * i
                acc[slot, i] = total[:, at : at + 128] + row

    project((3, 5), near[0:2])
    project((7, 1), (near[2], w.at[4]))
    project((0, 2), (w.at[0], w.at[1]))
    project((4, 6), (w.at[2], w.at[3]))

    def one(c, carry):
        base = c // 2 * 4 + 2 * lax.rem(k + c, 2)
        emit(out, acc[c, 0], acc[c, 1], acc[c, 2], [(base, 0), (16 + base, 32)], [(k * 16 + base, 64)])
        return carry

    lax.fori_loop(0, 2 * NX, one, 0)


def attn_kernel(layer, idx, order, mask, part_time, r_own, r_par, out, kt, vals, score, prob):
    mine = idx[2 + layer]
    low = lanes((128, 128)) < 64

    def place(at, block):
        key, val = block.astype(jnp.float32), block
        both = jnp.where(low, key, pltpu.roll(key, 64, 1))
        kt[0:128, at : at + 128] = both.T.astype(jnp.bfloat16)
        vals[at : at + 128, :] = jnp.where(low, jnp.ones_like(val), val)

    def queries(packed, which):
        scaled = packed * SCALE
        high = scaled.astype(jnp.bfloat16).astype(jnp.float32)
        rest = scaled - high
        left = jnp.where(lanes(packed.shape) < 64, high, pltpu.roll(rest, 64, 1))
        return jnp.concatenate([left.astype(jnp.bfloat16), which.astype(jnp.bfloat16)], axis=1)

    sub = lax.broadcasted_iota(jnp.int32, (PARTS, 8, 128), 1)
    tail_own = r_own[:, 48:56, :].astype(jnp.float32)
    tail_par = r_par[:, 48:56, :].astype(jnp.float32)
    extra = jnp.sum(jnp.where(sub == 0, jnp.where(mine == 1, tail_own, tail_par), 0.0), axis=1)
    place(0, jnp.concatenate([extra, jnp.zeros((96, 128), jnp.float32)], axis=0).astype(jnp.bfloat16))
    kt[128:144, :] = mask[...]
    kt[144:256, :] = jnp.zeros((112, KEYS), jnp.bfloat16)
    for t in range(FRAMES):
        at = pl.ds(2 * order[t], 2)
        own = r_own[at, 0:32, :].reshape(64, 128)
        par = r_par[at, 0:32, :].reshape(64, 128)
        place(128 * t + 128, jnp.concatenate([own, par], axis=0))

    def dots(lhs, rows, n, buf):
        score[buf, 0:rows, 0:n] = jnp.dot(lhs, kt[:, 0:n], preferred_element_type=jnp.float32)

    def soft(rows, n, buf):
        for r in range(0, rows, 16):
            now = score[buf, r : r + 16, 0:n]
            now = jnp.exp2(now - jnp.max(now, axis=1, keepdims=True))
            prob[buf, r : r + 16, 0:n] = now.astype(jnp.bfloat16)

    def mix(rows, n, buf):
        return jnp.dot(prob[buf, 0:rows, 0:n], vals[0:n, :], preferred_element_type=jnp.float32)

    row = lax.broadcasted_iota(jnp.int32, (256, 128), 0)
    lowh = lanes((128, 128)) < 64

    def lhs_of(i):
        packed = jnp.concatenate(
            [r_own[pl.ds(2 * order[4 * i + t], 2), 32:48, :].reshape(32, 128) for t in range(4)], axis=0
        ).astype(jnp.float32)
        packed = jnp.concatenate([packed, pltpu.roll(packed, 64, 1)], axis=0)
        which = jnp.where(lanes((256, 128)) == 4 * i + (row % 128) // 32, 1.0, 0.0)
        return queries(packed, which)

    def put(i, mixed):
        first, second = mixed[:128], mixed[128:]
        value = jnp.where(lowh, pltpu.roll(first, 64, 1), second)
        total = jnp.where(lowh, first, pltpu.roll(second, 64, 1))
        merged = (value / total).astype(jnp.bfloat16)
        for t in range(4):
            out[pl.ds(2 * order[4 * i + t], 2), 0:16, :] = merged[32 * t : 32 * t + 32].reshape(2, 16, 128)

    n_of = [128 + 128 * 4 * (i + 1) for i in range(4)]
    packed = jnp.sum(jnp.where(sub == 1, tail_own, 0.0), axis=1)
    which = jnp.where(lanes((PARTS, 128)) == part_time[...], 1.0, 0.0)
    cond = queries(packed, which)
    steps = [(lhs_of(i), 256, n_of[i]) for i in range(4)] + [(cond, PARTS, KEYS)]
    done = {}
    dots(*steps[0], 0)
    for i in range(len(steps) + 1):
        if i + 1 < len(steps):
            dots(*steps[i + 1], (i + 1) % 3)
        if i < len(steps):
            soft(*steps[i][1:], i % 3)
        if i >= 1:
            done[i - 1] = mix(*steps[i - 1][1:], (i - 1) % 3)
            if i - 1 < len(steps) - 1:
                put(i - 1, done[i - 1])

    res = done[4]
    res = pltpu.roll(res / pltpu.roll(res, 64, 1), 64, 1)
    out[:, 16:24, :] = jnp.broadcast_to(res[:, None, :], (PARTS, 8, 128)).astype(jnp.bfloat16)


def pair(first, second):
    low = lanes((24, 128)) < 64
    first, second = first.astype(jnp.float32), second.astype(jnp.float32)
    return (
        jnp.where(low, first, pltpu.roll(second, 64, 1)).astype(jnp.bfloat16),
        jnp.where(low, pltpu.roll(first, 64, 1), second).astype(jnp.bfloat16),
    )


def gather_heads(dst, at, back, patches, tail):
    for b, slot in enumerate(patches):
        lo, hi = pair(back[slot], back[slot + 1])
        dst[at + 32 * b : at + 32 * b + 16, :] = lo[:16]
        dst[at + 32 * b + 16 : at + 32 * b + 32, :] = hi[:16]
    lo, _ = pair(back[tail], back[tail + 1])
    dst[at + 64 : at + 72, :] = lo[16:24]


def heads_kernel(idx, back, out):
    k = idx[1]
    for c, side in enumerate((k, 1 - k)):
        for s in range(NX):
            slots = [s * 8 + b * 4 + 2 * side for b in range(2)]
            cols = slice(128 * c, 128 * c + 128)
            gather_heads(out.at[:, cols], PAD * s, back, slots, s * 8 + k * 4 + 2 * side)


def blocks_of(plane):
    return jnp.concatenate([plane[128 * j : 128 * j + 128, :] for j in range(8)], axis=1)


def every_out_kernel(h0, h1, h2, h3, xrows, o_bias, gain, bias, *rest):
    w, w_par, first, normed, lhs = rest
    for s, heads in enumerate((h0, h1, h2, h3)):
        for r in range(NX):
            at = PAD * ((r - s) % NX)
            lhs[PAD * r : PAD * r + PAD, 256 * s : 256 * s + 256] = heads[at : at + PAD, :]
    weight = jnp.concatenate(
        [blocks_of(p) for s in range(NX) for p in (w.at[s, 0], w_par.at[s, 0])], axis=0
    )
    total = jnp.dot(lhs[...], weight, preferred_element_type=jnp.float32)
    rows = xrows[...].astype(jnp.float32) + total + o_bias[0:1, :]
    first[...] = rows[0:65]
    normed[...] = norm(rows, gain[0:1, :], bias[0:1, :]).astype(jnp.bfloat16)


def whole_out_kernel(idx, back, own, o_bias, gain, bias, *rest):
    w, *near, first, normed, heads = rest
    k = idx[1]
    for s in range(NX):
        for c, side in enumerate((k, 1 - k)):
            base = s * 4 + 2 * side
            at = 256 * s + 128 * c
            gather_heads(heads.at[:, at : at + 128], 0, back, [base, 16 + base], k * 16 + base)
    weight = jnp.concatenate(
        [blocks_of(p) for s in range(NX) for p in (w.at[s, 0], near[s - 1].at[3] if s else w.at[4, 0])], axis=0
    )
    total = jnp.dot(heads[...], weight, preferred_element_type=jnp.float32)
    rows = own[...].astype(jnp.float32) + total[:65] + o_bias[1:2, :]
    first[...] = rows
    normed[...] = norm(rows, gain[1:2, :], bias[1:2, :]).astype(jnp.bfloat16)


def mlp_kernel(group, n, w1_own, w1_par, b1_own, b1_par, w2_own, w2_par, *rest):
    outs, rows = rest[:-1], rest[-1]
    for c, s in enumerate(group):
        rows[PAD * c : PAD * c + PAD, :] = n[PAD * s : PAD * s + PAD, :]
    total = None
    for w1, b1, w2 in ((w1_own, b1_own, w2_own), (w1_par.at[0], b1_par, w2_par.at[0])):
        inner = jnp.dot(rows[...], w1[...], preferred_element_type=jnp.float32) + b1[0:1, :]
        inner = (0.5 * inner * (1.0 + lax.erf(inner * 0.7071067811865476))).astype(jnp.bfloat16)
        part = jnp.dot(inner, w2[...], preferred_element_type=jnp.float32)
        total = part if total is None else total + part
    for c, y in enumerate(outs):
        y[...] = total[PAD * c : PAD * c + 65].astype(jnp.bfloat16)


def hidden(rows, w1, b1):
    inner = jnp.dot(rows, w1, preferred_element_type=jnp.float32) + b1
    return (0.5 * inner * (1.0 + lax.erf(inner * 0.7071067811865476))).astype(jnp.bfloat16)


def add_mlp(total, rows, *shares):
    for w in shares:
        bias = jnp.sum(w[0, D:HELD, :].astype(jnp.float32), axis=0, keepdims=True)
        inner = hidden(rows, w[0, 0:D, :], bias)
        part = jnp.concatenate(
            [
                jnp.dot(inner, w[1, 512 * j : 512 * j + 512, :], preferred_element_type=jnp.float32)
                for j in range(2)
            ],
            axis=1,
        )
        total = part if total is None else total + part
    return total


def core_mlp(rows, w1_par, b1_par, w2_par):
    return jnp.dot(hidden(rows, w1_par[1], b1_par[1:2, :]), w2_par[1], preferred_element_type=jnp.float32)


def near_mlp_kernel(first, n, packed, w1_par, b1_par, w2_par, o_bias, total, rows):
    rows[0:65, :] = n[...]
    share = add_mlp(core_mlp(rows[...], w1_par, b1_par, w2_par), rows[...], packed)
    total[...] = first[...] + share[:65] + o_bias[1:2, :]


def far_mlp_kernel(idx, n, near, far, far_par, keep, send, rows):
    k = idx[1]
    rows[0:65, :] = n[...]
    share = add_mlp(None, rows[...], far, far_par)
    total = near[...] + share[:65]
    keep[...] = total
    send[...] = jnp.where(k == 0, total[32:64], total[0:32])


def pair_mlp_kernel(idx, n, packed, w1_par, b1_par, w2_par, far, far_par, here, there, rows):
    k = idx[1]
    rows[0:65, :] = n[...]
    total = core_mlp(rows[...], w1_par, b1_par, w2_par)
    total = add_mlp(total, rows[...], packed, far, far_par).astype(jnp.bfloat16)
    here[0:32, :] = jnp.where(k == 0, total[0:32], total[32:64])
    here[32:40, :] = total[64:72]
    there[...] = jnp.where(k == 0, total[32:64], total[0:32])


def last_kernel(idx, keep, other, here, there, out):
    k = idx[1]
    mine = jnp.where(k == 0, keep[0:32, :], keep[32:64, :]) + here[0:32, :].astype(jnp.float32)
    theirs = other[...] + there[...].astype(jnp.float32)
    out[0, 0:32, :] = jnp.where(k == 0, mine, theirs).astype(jnp.bfloat16)
    out[0, 32:64, :] = jnp.where(k == 0, theirs, mine).astype(jnp.bfloat16)
    out[0, 64:65, :] = (keep[64:65, :] + here[32:33, :].astype(jnp.float32)).astype(jnp.bfloat16)


VMEM = pl.BlockSpec(memory_space=pltpu.VMEM)
SMEM = pl.BlockSpec(memory_space=pltpu.SMEM)
HBM = pl.BlockSpec(memory_space=pltpu.HBM)


def block(dtype=jnp.bfloat16, rows=BLOCK):
    return jax.ShapeDtypeStruct((rows, D), dtype)


def call(kernel, args, out_shape, scratch=(), scalars=1, limit=8, out_specs=None, in_specs=None, aliases=None):
    return pl.pallas_call(
        kernel,
        out_shape=out_shape,
        in_specs=in_specs or [SMEM] * scalars + [VMEM] * (len(args) - scalars),
        out_specs=out_specs or ([VMEM] * len(out_shape) if isinstance(out_shape, list) else VMEM),
        scratch_shapes=list(scratch),
        input_output_aliases=aliases or {},
        compiler_params=pltpu.CompilerParams(vmem_limit_bytes=limit << 20),
    )(*args)


def shards(
    frames_in,
    frame_time,
    cond_count,
    ln1_gain,
    ln1_bias,
    qkv_weight,
    qkv_bias,
    out_weight,
    out_bias,
    ln2_gain,
    ln2_bias,
    fc1_weight,
    fc1_bias,
    fc2_weight,
    fc2_bias,
):
    part = lax.axis_index("tm")
    pos = lax.axis_index("tensor")
    x, k = pos // 2, pos % 2

    def shift(array, s):
        pairs = [(t, ((t // 2 + s) % NX) * 2 + t % 2) for t in range(2 * NX)]
        return lax.ppermute(array, "tensor", pairs)

    def swap(array):
        return lax.ppermute(array, "tensor", [(t, t ^ 1) for t in range(2 * NX)])

    def spread(array):
        return [array] + [shift(array, -s) for s in (1, 2, 3)]

    def collect(parts):
        return [parts[0]] + [shift(parts[s], s) for s in (1, 2, 3)]

    tie = lax.optimization_barrier

    seen = []

    def attention(layer, message, beside, *late, ahead=()):
        arrived = lax.all_to_all(message, "tm", 0, 0, tiled=True)
        arrived, *late = tie((arrived, *late))
        arrived_par = swap(arrived)
        seen.append(beside())
        order, mask, row_time = seen[0]
        arrived, arrived_par, *late = tie((arrived, arrived_par, *late))
        late = [swap(a) for a in late]
        mixed = call(
            functools.partial(attn_kernel, layer),
            (idx, order, mask, row_time, arrived, arrived_par),
            jax.ShapeDtypeStruct((PARTS, 24, 128), jnp.bfloat16),
            [
                pltpu.VMEM((256, KEYS), jnp.bfloat16),
                pltpu.VMEM((KEYS, 128), jnp.bfloat16),
                pltpu.VMEM((3, 256, KEYS), jnp.float32),
                pltpu.VMEM((3, 256, KEYS), jnp.bfloat16),
            ],
            scalars=2,
            limit=24,
        )
        mixed, *late = tie((mixed, *late, *ahead))
        back = lax.all_to_all(mixed, "tm", 0, 0, tiled=True)
        return tie((back, *late))

    message_shape = jax.ShapeDtypeStruct((PARTS, 56, 128), jnp.bfloat16)

    def in_hbm(*arrays):
        return [pltpu.with_memory_space_constraint(a, pltpu.HBM) for a in arrays]

    biases = jnp.transpose(qkv_bias, (1, 0, 2))
    idx = jnp.stack([x, k, k == (part // 4) % 2, k == part // 16]).astype(jnp.int32)
    held = call(
        pack_kernel,
        in_hbm(qkv_weight, out_weight, biases),
        jax.ShapeDtypeStruct((5, HELD, 128), jnp.bfloat16),
        [pltpu.VMEM((3, LAYERS, 128), jnp.float32), pltpu.SemaphoreType.DMA((18,))],
        in_specs=[HBM] * 3,
    )
    held, late_qkv, late_biases, late_fc2 = tie((held, qkv_weight, biases, fc2_weight))
    qkv_par = swap(late_qkv)
    biases_par = swap(late_biases)
    fc2_par = swap(late_fc2)
    helds = spread(held)
    held_par = swap(held)
    xrows, message = call(
        start_kernel,
        (idx, *in_hbm(frames_in, qkv_weight, qkv_par, biases), biases_par, *in_hbm(ln1_gain, ln1_bias)),
        [block(rows=NX * PAD), message_shape],
        [
            pltpu.VMEM((8 * BLOCK, D), jnp.bfloat16),
            pltpu.VMEM((8 * BLOCK, D), jnp.float32),
            pltpu.VMEM((NX * PAD, D), jnp.bfloat16),
            pltpu.VMEM((2, 3, D, 128), jnp.bfloat16),
            pltpu.VMEM((3, LAYERS, 128), jnp.float32),
            pltpu.VMEM((2, LAYERS, D), jnp.float32),
            pltpu.SemaphoreType.DMA((6,)),
        ],
        in_specs=[SMEM, HBM, HBM, HBM, HBM, VMEM, HBM, HBM],
        limit=12,
    )
    message = tie(message)

    def tables():
        return call(
            tables_kernel,
            (frame_time, cond_count),
            [
                jax.ShapeDtypeStruct((FRAMES,), jnp.int32),
                jax.ShapeDtypeStruct((FRAMES, KEYS), jnp.bfloat16),
                jax.ShapeDtypeStruct((PARTS, 128), jnp.int32),
            ],
            scalars=2,
            out_specs=[SMEM, VMEM, VMEM],
        )

    def load(planes, count, refs):
        return call(
            functools.partial(load_kernel, planes),
            refs,
            jax.ShapeDtypeStruct((len(refs), count, HELD, 128), jnp.bfloat16),
            [pltpu.SemaphoreType.DMA((len(refs),))],
            in_specs=[HBM] * len(refs),
        )

    back, fc1_par, fc1_bias_par, fc2_par, held_par = attention(
        0, message, tables, fc1_weight, fc1_bias, ahead=(fc2_par, held_par)
    )
    heads = call(heads_kernel, (idx, back), jax.ShapeDtypeStruct((NX * PAD, 256), jnp.bfloat16))
    heads = spread(heads)
    packed, w1, w2 = call(
        load_mlp_kernel,
        in_hbm(fc1_weight, fc1_bias, fc2_weight),
        [
            jax.ShapeDtypeStruct((2, HELD, 512), jnp.bfloat16),
            jax.ShapeDtypeStruct((D, 512), jnp.bfloat16),
            jax.ShapeDtypeStruct((512, D), jnp.bfloat16),
        ],
        [pltpu.VMEM((LAYERS, 512), jnp.float32), pltpu.SemaphoreType.DMA((6,))],
        in_specs=[HBM] * 3,
    )
    loaded = load(slice(4, 5), 1, in_hbm(*helds))
    loaded_par = swap(loaded)
    held_pars = [held_par] + [swap(helds[s]) for s in (1, 2, 3)]
    far_refs = in_hbm(*helds, held_pars[0])
    near = held_pars[1:]
    first, normed_two = call(
        every_out_kernel,
        (*heads, xrows, out_bias, ln2_gain, ln2_bias, loaded, loaded_par),
        [block(jnp.float32), block(rows=NX * PAD)],
        [pltpu.VMEM((NX * PAD, D), jnp.bfloat16)],
        scalars=0,
    )
    partial = {}
    for group in GROUPS:
        done = call(
            functools.partial(mlp_kernel, group),
            (normed_two, w1, fc1_par, fc1_bias, fc1_bias_par, w2, fc2_par),
            [block()] * len(group),
            [pltpu.VMEM((PAD * len(group), D), jnp.bfloat16)],
            scalars=0,
        )
        partial.update(zip(group, done))

    def pair(array, other):
        return lax.ppermute(array, "tensor", [(t, other(t // 2) * 2 + t % 2) for t in range(2 * NX)])

    far = pair(packed, lambda c: c ^ 1)
    loaded = load(slice(0, 3), 3, far_refs)
    partial = collect(partial)
    stream, message = call(
        turn_kernel,
        (idx, first, *partial, fc2_bias, ln1_gain, ln1_bias, loaded, *near),
        [block(), message_shape],
        [pltpu.VMEM((PAD, D), jnp.bfloat16), pltpu.VMEM((2 * NX, 3, PAD, 128), jnp.float32)],
    )
    (back,) = attention(1, message, lambda: load(slice(3, 4), 1, far_refs))
    back, far, loaded = tie((back, far, seen[1]))
    far_par = swap(far)
    first, normed_two = call(
        whole_out_kernel,
        (idx, back, stream, out_bias, ln2_gain, ln2_bias, loaded, *near),
        [block(jnp.float32), block()],
        [pltpu.VMEM((PAD, D), jnp.bfloat16)],
    )
    moved = pair(normed_two, lambda c: 3 - c)
    pad = [pltpu.VMEM((PAD, D), jnp.bfloat16)]
    weights = (packed, fc1_par, fc1_bias_par, fc2_par)
    total = call(
        near_mlp_kernel,
        (first, normed_two, *weights, fc2_bias),
        block(jnp.float32),
        pad,
        scalars=0,
    )
    keep, send = call(
        far_mlp_kernel,
        (idx, normed_two, total, far, far_par),
        [block(jnp.float32), block(jnp.float32, 32)],
        pad,
    )
    other = swap(send)
    here, there = call(pair_mlp_kernel, (idx, moved, *weights, far, far_par), [block(rows=40), block(rows=32)], pad)
    here = pair(here, lambda c: 3 - c)
    cross = [(t, (3 - t // 2) * 2 + 1 - t % 2) for t in range(2 * NX)]
    there = lax.ppermute(there, "tensor", cross)
    return call(
        last_kernel, (idx, keep, other, here, there), jax.ShapeDtypeStruct((1, BLOCK, D), jnp.bfloat16)
    )


def solution(mesh):
    in_specs = (
        P("tm", None, None),
        P(),
        P(),
        P(),
        P(),
        P(None, None, None, "tensor"),
        P(None, None, "tensor"),
        P(None, "tensor", None),
        P(),
        P(),
        P(),
        P(None, None, "tensor"),
        P(None, "tensor"),
        P(None, "tensor", None),
        P(),
    )
    out_specs = P("tm", "tensor", None)
    return jax.shard_map(shards, mesh=mesh, in_specs=in_specs, out_specs=out_specs, check_vma=False)
```

```python
import functools

import jax
import jax.numpy as jnp
from jax import lax
from jax.experimental import pallas as pl
from jax.experimental.pallas import tpu as pltpu
from jax.sharding import PartitionSpec as P

D = 1024
LAYERS = 2
PARTS = 32
FRAMES = 16
BLOCK = 65
PAD = 72
KEYS = 2176
NX = 4
HELD = 1032
LOG2E = 1.4426950408889634
SCALE = 0.125 * LOG2E
NEG = -1e30

GROUPS = ((1, 3, 2, 0),)


def core_index():
    return lax.rem(lax.axis_index("tensor"), 2)


def lanes(shape):
    return lax.broadcasted_iota(jnp.int32, shape, len(shape) - 1)


def subs(shape):
    return lax.broadcasted_iota(jnp.int32, shape, len(shape) - 2)


def norm(rows, gain, bias):
    center = jnp.mean(rows, axis=-1, keepdims=True)
    off = rows - center
    spread = jnp.mean(off * off, axis=-1, keepdims=True)
    return off * lax.rsqrt(spread + 1e-06) * gain + bias


def pack_kernel(w_ref, wo_ref, bias_ref, x_ref, held, wide, raw, w, biases, sems):
    copies = [
        pltpu.make_async_copy(w_ref.at[1], held.at[0:3, 0:D, :], sems.at[0]),
        pltpu.make_async_copy(bias_ref, biases, sems.at[1]),
    ]
    for j in range(8):
        cols = slice(128 * j, 128 * j + 128)
        copies.append(pltpu.make_async_copy(wo_ref.at[0, :, cols], held.at[3, cols, :], sems.at[2 + j]))
        copies.append(pltpu.make_async_copy(wo_ref.at[1, :, cols], wide.at[cols, :], sems.at[10 + j]))
    copies.append(pltpu.make_async_copy(x_ref.at[0], raw, sems.at[18]))
    copies.append(pltpu.make_async_copy(w_ref.at[0], w, sems.at[19]))
    for copy in copies:
        copy.start()
    for copy in copies:
        copy.wait()
    for i in range(3):
        held[i, D:HELD, :] = split_rows(biases[i, 1:2, :])
    held[3, D:HELD, :] = jnp.zeros((8, 128), jnp.bfloat16)


def tables_kernel(frame_time, cond_count, order, mask, row_time):
    for f in range(FRAMES):
        order[frame_time[f]] = f
    slot_time = jnp.full((FRAMES, 128), FRAMES, jnp.int32)
    times = jnp.zeros((PARTS, 128), jnp.int32)
    for g in range(PARTS):
        time = frame_time[g // 2]
        seen = jnp.where(g % 2 < cond_count[g // 2], time, FRAMES)
        slot_time = jnp.where(lanes(slot_time.shape) == g, seen, slot_time)
        times = jnp.where(subs(times.shape) == g, time, times)
    row_time[...] = times
    mask[:, 0:128] = jnp.where(slot_time <= subs(slot_time.shape), 0.0, NEG).astype(jnp.bfloat16)
    for t in range(FRAMES):
        seen = jnp.where(subs((FRAMES, 128)) >= t, 0.0, NEG)
        mask[:, 128 * t + 128 : 128 * t + 256] = seen.astype(jnp.bfloat16)


def plane_kernel(h0, h1, h2, h3, out):
    for c, held in enumerate((h0, h1, h2, h3)):
        out[c] = held[3, 0:D]


def stack_kernel(w0, w1, w2, w3, out):
    for c, w in enumerate((w0, w1, w2, w3)):
        out[c] = w[...]


def load_mlp_kernel(w1_ref, b1_ref, w2_ref, packed_a, packed_b, w1, w2, bias, sems):
    copies = [
        pltpu.make_async_copy(w1_ref.at[0], w1, sems.at[0]),
        pltpu.make_async_copy(w2_ref.at[0], w2, sems.at[1]),
        pltpu.make_async_copy(b1_ref, bias, sems.at[2]),
    ]
    for h, packed in enumerate((packed_a, packed_b)):
        units = slice(256 * h, 256 * h + 256)
        copies.append(pltpu.make_async_copy(w1_ref.at[1, :, units], packed.at[0, 0:D], sems.at[3 + 5 * h]))
        for j in range(4):
            cols = slice(256 * j, 256 * j + 256)
            copies.append(
                pltpu.make_async_copy(w2_ref.at[1, units, cols], packed.at[1, cols], sems.at[4 + 5 * h + j])
            )
    for copy in copies:
        copy.start()
    for copy in copies:
        copy.wait()
    for h, packed in enumerate((packed_a, packed_b)):
        packed[0, D:HELD, :] = split_rows(bias[1:2, 256 * h : 256 * h + 256])
        packed[1, D:HELD, :] = jnp.zeros((8, 256), jnp.bfloat16)


def split_rows(row):
    high = row.astype(jnp.bfloat16).astype(jnp.float32)
    middle = (row - high).astype(jnp.bfloat16).astype(jnp.float32)
    lowest = (row - high) - middle
    sub = subs((8, row.shape[1]))
    rows = jnp.where(sub == 0, high, jnp.where(sub == 1, middle, jnp.where(sub == 2, lowest, 0.0)))
    return rows.astype(jnp.bfloat16)


def from_row(ref, base, off, count):
    return pltpu.roll(ref[pl.ds(pl.multiple_of(base, 8), count), :], lax.rem(count - off, count), 0)


def emit(out, q, key, val, places, tails):
    low = lanes(q.shape) < 64
    low8 = lanes((8, 128)) < 64
    sub = lax.broadcasted_iota(jnp.int32, (8, 128), 0)
    q_r, key_r, val_r = (pltpu.roll(a, 64, 1) for a in (q, key, val))
    for hl in range(2):
        if hl == 0:
            kv = jnp.where(low, key, val_r)
            q_lo, q_hi = q, q_r
        else:
            kv = jnp.where(low, key_r, val)
            q_lo, q_hi = q_r, q
        for slot, at in places:
            out[slot + hl, 0:32, :] = kv[at : at + 32].astype(jnp.bfloat16)
            out[slot + hl, 32:48, :] = jnp.where(
                low[:16], q_lo[at : at + 16], q_hi[at + 16 : at + 32]
            ).astype(jnp.bfloat16)
            out[slot + hl, 48:56, :] = jnp.zeros((8, 128), jnp.bfloat16)
        for slot, at in tails:
            tail = jnp.where(
                sub == 0,
                jnp.broadcast_to(kv[at : at + 1], (8, 128)),
                jnp.where((sub == 1) & low8, jnp.broadcast_to(q_lo[at : at + 1], (8, 128)), 0.0),
            )
            out[slot + hl, 48:56, :] = tail.astype(jnp.bfloat16)


def start_kernel(x_ref, w_own, w_par, b_own, b_par, g_ref, b_ref, xrows, out, wide, rows):
    x, k = lax.axis_index("tensor") // 2, core_index()
    wide[...] = x_ref[...].astype(jnp.float32)
    gain, bias = g_ref[0:1, :], b_ref[0:1, :]
    for s in range(NX):
        chip = lax.rem(x + s, NX)
        for b in range(2):
            part = from_row(wide, 64 * (2 * chip + b) + 32 * k, 2 * chip + b, 40)[:32]
            at = PAD * s + 32 * b
            rows[at : at + 32, :] = norm(part, gain, bias).astype(jnp.bfloat16)
            xrows[at : at + 32, :] = part.astype(jnp.bfloat16)
        part = from_row(wide, 64 * (2 * chip + k) + 64, 2 * chip + k, 8)
        at = PAD * s + 64
        rows[at : at + 8, :] = norm(part, gain, bias).astype(jnp.bfloat16)
        xrows[at : at + 8, :] = part.astype(jnp.bfloat16)
    both = jnp.concatenate([w[i] for w in (w_own, w_par.at[0]) for i in range(3)], axis=1)
    both = jnp.dot(rows[...], both, preferred_element_type=jnp.float32)
    for c, (side, row) in enumerate(((k, b_own), (1 - k, b_par))):
        places = [(s * 8 + b * 4 + 2 * side, PAD * s + 32 * b) for s in range(NX) for b in range(2)]
        tails = [(s * 8 + k * 4 + 2 * side, PAD * s + 64) for s in range(NX)]
        parts = [both[:, 384 * c + 128 * i : 384 * c + 128 * i + 128] + row[i, 0:1, :] for i in range(3)]
        emit(out, *parts, places, tails)


def turn_kernel(first, y0, y1, y2, y3, o_bias, gain, bias, *rest):
    owns, pars, (stream, out, rows, acc) = rest[:NX], rest[NX : 2 * NX], rest[2 * NX :]
    k = core_index()
    summed = (y0[...].astype(jnp.float32) + y1[...].astype(jnp.float32)) + (
        y2[...].astype(jnp.float32) + y3[...].astype(jnp.float32)
    )
    new = (first[...] + summed + o_bias[0:1, :]).astype(jnp.bfloat16)
    stream[...] = new
    rows[0:65, :] = norm(new.astype(jnp.float32), gain[1:2, :], bias[1:2, :]).astype(jnp.bfloat16)

    def project(slots, refs):
        weight = jnp.concatenate([ref[i, 0:D, :] for ref in refs for i in range(3)], axis=1)
        total = jnp.dot(rows[...], weight, preferred_element_type=jnp.float32)
        for c, (slot, ref) in enumerate(zip(slots, refs)):
            for i in range(3):
                row = jnp.sum(ref[i, D:HELD, :].astype(jnp.float32), axis=0, keepdims=True)
                at = 384 * c + 128 * i
                acc[slot, i] = total[:, at : at + 128] + row

    for s in range(NX):
        project((2 * s, 2 * s + 1), (owns[s], pars[s]))

    def one(c, carry):
        base = c // 2 * 4 + 2 * lax.rem(k + c, 2)
        emit(out, acc[c, 0], acc[c, 1], acc[c, 2], [(base, 0), (16 + base, 32)], [(k * 16 + base, 64)])
        return carry

    lax.fori_loop(0, 2 * NX, one, 0)


def attn_kernel(layer, order, mask, part_time, r_own, r_par, out, kt, vals, score, prob):
    slot = lax.axis_index("tm")
    slot_core = lax.rem(slot // 4, 2) if layer == 0 else slot // 16
    mine = jnp.where(core_index() == slot_core, 1, 0)
    low = lanes((128, 128)) < 64

    def place(at, block):
        key, val = block.astype(jnp.float32), block
        both = jnp.where(low, key, pltpu.roll(key, 64, 1))
        kt[0:128, at : at + 128] = both.T.astype(jnp.bfloat16)
        vals[at : at + 128, :] = jnp.where(low, jnp.ones_like(val), val)

    def queries(packed, which):
        scaled = packed * SCALE
        high = scaled.astype(jnp.bfloat16).astype(jnp.float32)
        rest = scaled - high
        left = jnp.where(lanes(packed.shape) < 64, high, pltpu.roll(rest, 64, 1))
        return jnp.concatenate([left.astype(jnp.bfloat16), which.astype(jnp.bfloat16)], axis=1)

    sub = lax.broadcasted_iota(jnp.int32, (PARTS, 8, 128), 1)
    tail_own = r_own[:, 48:56, :].astype(jnp.float32)
    tail_par = r_par[:, 48:56, :].astype(jnp.float32)
    extra = jnp.sum(jnp.where(sub == 0, jnp.where(mine == 1, tail_own, tail_par), 0.0), axis=1)
    place(0, jnp.concatenate([extra, jnp.zeros((96, 128), jnp.float32)], axis=0).astype(jnp.bfloat16))
    kt[128:144, :] = mask[...]
    kt[144:256, :] = jnp.zeros((112, KEYS), jnp.bfloat16)
    for t in range(FRAMES):
        at = pl.ds(2 * order[t], 2)
        own = r_own[at, 0:32, :].reshape(64, 128)
        par = r_par[at, 0:32, :].reshape(64, 128)
        place(128 * t + 128, jnp.concatenate([own, par], axis=0))

    def dots(lhs, rows, n, buf):
        score[buf, 0:rows, 0:n] = jnp.dot(lhs, kt[:, 0:n], preferred_element_type=jnp.float32)

    def soft(rows, n, buf):
        for r in range(0, rows, 16):
            now = score[buf, r : r + 16, 0:n]
            now = jnp.exp2(now - jnp.max(now, axis=1, keepdims=True))
            prob[buf, r : r + 16, 0:n] = now.astype(jnp.bfloat16)

    def mix(rows, n, buf):
        return jnp.dot(prob[buf, 0:rows, 0:n], vals[0:n, :], preferred_element_type=jnp.float32)

    row = lax.broadcasted_iota(jnp.int32, (256, 128), 0)
    lowh = lanes((128, 128)) < 64

    def lhs_of(i):
        packed = jnp.concatenate(
            [r_own[pl.ds(2 * order[4 * i + t], 2), 32:48, :].reshape(32, 128) for t in range(4)], axis=0
        ).astype(jnp.float32)
        packed = jnp.concatenate([packed, pltpu.roll(packed, 64, 1)], axis=0)
        which = jnp.where(lanes((256, 128)) == 4 * i + (row % 128) // 32, 1.0, 0.0)
        return queries(packed, which)

    def put(i, mixed):
        first, second = mixed[:128], mixed[128:]
        value = jnp.where(lowh, pltpu.roll(first, 64, 1), second)
        total = jnp.where(lowh, first, pltpu.roll(second, 64, 1))
        merged = (value / total).astype(jnp.bfloat16)
        for t in range(4):
            out[pl.ds(2 * order[4 * i + t], 2), 0:16, :] = merged[32 * t : 32 * t + 32].reshape(2, 16, 128)

    n_of = [128 + 128 * 4 * (i + 1) for i in range(4)]
    packed = jnp.sum(jnp.where(sub == 1, tail_own, 0.0), axis=1)
    which = jnp.where(lanes((PARTS, 128)) == part_time[...], 1.0, 0.0)
    cond = queries(packed, which)
    steps = [(lhs_of(i), 256, n_of[i]) for i in range(4)] + [(cond, PARTS, KEYS)]
    done = {}
    dots(*steps[0], 0)
    for i in range(len(steps) + 1):
        if i + 1 < len(steps):
            dots(*steps[i + 1], (i + 1) % 3)
        if i < len(steps):
            soft(*steps[i][1:], i % 3)
        if i >= 1:
            done[i - 1] = mix(*steps[i - 1][1:], (i - 1) % 3)
            if i - 1 < len(steps) - 1:
                put(i - 1, done[i - 1])

    res = done[4]
    res = pltpu.roll(res / pltpu.roll(res, 64, 1), 64, 1)
    out[:, 16:24, :] = jnp.broadcast_to(res[:, None, :], (PARTS, 8, 128)).astype(jnp.bfloat16)


def pair(first, second):
    low = lanes((24, 128)) < 64
    first, second = first.astype(jnp.float32), second.astype(jnp.float32)
    return (
        jnp.where(low, first, pltpu.roll(second, 64, 1)).astype(jnp.bfloat16),
        jnp.where(low, pltpu.roll(first, 64, 1), second).astype(jnp.bfloat16),
    )


def gather_heads(dst, at, back, patches, tail):
    for b, slot in enumerate(patches):
        lo, hi = pair(back[slot], back[slot + 1])
        dst[at + 32 * b : at + 32 * b + 16, :] = lo[:16]
        dst[at + 32 * b + 16 : at + 32 * b + 32, :] = hi[:16]
    lo, _ = pair(back[tail], back[tail + 1])
    dst[at + 64 : at + 72, :] = lo[16:24]


def heads_kernel(back, out):
    k = core_index()
    for c, side in enumerate((k, 1 - k)):
        for s in range(NX):
            slots = [s * 8 + b * 4 + 2 * side for b in range(2)]
            cols = slice(128 * c, 128 * c + 128)
            gather_heads(out.at[:, cols], PAD * s, back, slots, s * 8 + k * 4 + 2 * side)


def blocks_of(plane):
    return jnp.concatenate([plane[128 * j : 128 * j + 128, :] for j in range(8)], axis=1)


def every_out_kernel(h0, h1, h2, h3, xrows, o_bias, gain, bias, *rest):
    w, w_par, first, normed, lhs = rest
    for s, heads in enumerate((h0, h1, h2, h3)):
        for r in range(NX):
            at = PAD * ((r - s) % NX)
            lhs[PAD * r : PAD * r + PAD, 256 * s : 256 * s + 256] = heads[at : at + PAD, :]
    weight = jnp.concatenate(
        [blocks_of(p) for s in range(NX) for p in (w.at[s], w_par.at[s])], axis=0
    )
    total = jnp.dot(lhs[...], weight, preferred_element_type=jnp.float32)
    rows = xrows[...].astype(jnp.float32) + total + o_bias[0:1, :]
    first[...] = rows[0:65]
    normed[...] = norm(rows, gain[0:1, :], bias[0:1, :]).astype(jnp.bfloat16)


def whole_out_kernel(back, own, o_bias, gain, bias, *rest):
    w, w_par, first, normed, heads = rest
    k = core_index()
    for s in range(NX):
        for c, side in enumerate((k, 1 - k)):
            base = s * 4 + 2 * side
            at = 256 * s + 128 * c
            gather_heads(heads.at[:, at : at + 128], 0, back, [base, 16 + base], k * 16 + base)
    weight = jnp.concatenate(
        [blocks_of(p.at[s]) for s in range(NX) for p in (w, w_par)], axis=0
    )
    total = jnp.dot(heads[...], weight, preferred_element_type=jnp.float32)
    rows = own[...].astype(jnp.float32) + total[:65] + o_bias[1:2, :]
    first[...] = rows
    normed[...] = norm(rows, gain[1:2, :], bias[1:2, :]).astype(jnp.bfloat16)


def mlp_kernel(group, n, w1_own, w1_par, b1_own, b1_par, w2_own, w2_par, *rest):
    outs, rows = rest[:-1], rest[-1]
    for c, s in enumerate(group):
        rows[PAD * c : PAD * c + PAD, :] = n[PAD * s : PAD * s + PAD, :]
    total = None
    for w1, b1, w2 in ((w1_own, b1_own, w2_own), (w1_par.at[0], b1_par, w2_par.at[0])):
        inner = jnp.dot(rows[...], w1[...], preferred_element_type=jnp.float32) + b1[0:1, :]
        inner = (0.5 * inner * (1.0 + lax.erf(inner * 0.7071067811865476))).astype(jnp.bfloat16)
        part = jnp.dot(inner, w2[...], preferred_element_type=jnp.float32)
        total = part if total is None else total + part
    for c, y in enumerate(outs):
        y[...] = total[PAD * c : PAD * c + 65].astype(jnp.bfloat16)


def hidden(rows, w1, b1):
    inner = jnp.dot(rows, w1, preferred_element_type=jnp.float32) + b1
    return (0.5 * inner * (1.0 + lax.erf(inner * 0.7071067811865476))).astype(jnp.bfloat16)


def add_mlp(total, rows, *shares):
    for w in shares:
        bias = jnp.sum(w[0, D:HELD, :].astype(jnp.float32), axis=0, keepdims=True)
        inner = hidden(rows, w[0, 0:D, :], bias)
        part = jnp.concatenate(
            [
                jnp.dot(inner, w[1, 256 * j : 256 * j + 256, :], preferred_element_type=jnp.float32)
                for j in range(4)
            ],
            axis=1,
        )
        total = part if total is None else total + part
    return total


def core_mlp(rows, w1_par, b1_par, w2_par):
    return jnp.dot(hidden(rows, w1_par[1], b1_par[1:2, :]), w2_par[1], preferred_element_type=jnp.float32)


def own_mlp_kernel(first, n, o_bias, w1_par, b1_par, w2_par, own_a, own_b, far_a, total, rows):
    rows[0:65, :] = n[...]
    share = core_mlp(rows[...], w1_par, b1_par, w2_par)
    share = add_mlp(share, rows[...], own_a, own_b, far_a)
    total[...] = first[...] + share[:65] + o_bias[1:2, :]


def half_mlp_kernel(total, n, far_b, far_a_par, out, rows):
    rows[0:65, :] = n[...]
    out[...] = total[...] + add_mlp(None, rows[...], far_b, far_a_par)[:65]


def moved_mlp_kernel(n, w1_par, b1_par, w2_par, own_a, own_b, far_a, far_a_par, far_b, total, rows):
    rows[0:65, :] = n[...]
    share = core_mlp(rows[...], w1_par, b1_par, w2_par)
    total[...] = add_mlp(share, rows[...], own_a, own_b, far_a, far_a_par, far_b)


def end_mlp_kernel(mine, moved, n, m, far_b_par, keep, send, here, there, rows):
    k = core_index()
    rows[0:65, :] = n[...]
    rows[PAD : PAD + 65, :] = m[...]
    share = add_mlp(None, rows[...], far_b_par)
    total = mine[...] + share[:65]
    keep[...] = total
    send[...] = jnp.where(k == 0, total[32:64], total[0:32])
    total = (moved[...] + share[PAD:]).astype(jnp.bfloat16)
    here[0:32, :] = jnp.where(k == 0, total[0:32], total[32:64])
    here[32:40, :] = total[64:72]
    there[...] = jnp.where(k == 0, total[32:64], total[0:32])


def last_kernel(keep, other, here, there, out):
    k = core_index()
    mine = jnp.where(k == 0, keep[0:32, :], keep[32:64, :]) + here[0:32, :].astype(jnp.float32)
    theirs = other[...] + there[...].astype(jnp.float32)
    out[0, 0:32, :] = jnp.where(k == 0, mine, theirs).astype(jnp.bfloat16)
    out[0, 32:64, :] = jnp.where(k == 0, theirs, mine).astype(jnp.bfloat16)
    out[0, 64:65, :] = (keep[64:65, :] + here[32:33, :].astype(jnp.float32)).astype(jnp.bfloat16)


VMEM = pl.BlockSpec(memory_space=pltpu.VMEM)
SMEM = pl.BlockSpec(memory_space=pltpu.SMEM)
HBM = pl.BlockSpec(memory_space=pltpu.HBM)


def block(dtype=jnp.bfloat16, rows=BLOCK):
    return jax.ShapeDtypeStruct((rows, D), dtype)


def call(kernel, args, out_shape, scratch=(), scalars=0, limit=8, out_specs=None, in_specs=None, aliases=None):
    return pl.pallas_call(
        kernel,
        out_shape=out_shape,
        in_specs=in_specs or [SMEM] * scalars + [VMEM] * (len(args) - scalars),
        out_specs=out_specs or ([VMEM] * len(out_shape) if isinstance(out_shape, list) else VMEM),
        scratch_shapes=list(scratch),
        input_output_aliases=aliases or {},
        compiler_params=pltpu.CompilerParams(vmem_limit_bytes=limit << 20),
    )(*args)


def shards(
    frames_in,
    frame_time,
    cond_count,
    ln1_gain,
    ln1_bias,
    qkv_weight,
    qkv_bias,
    out_weight,
    out_bias,
    ln2_gain,
    ln2_bias,
    fc1_weight,
    fc1_bias,
    fc2_weight,
    fc2_bias,
):
    def shift(array, s):
        pairs = [(t, ((t // 2 + s) % NX) * 2 + t % 2) for t in range(2 * NX)]
        return lax.ppermute(array, "tensor", pairs)

    def swap(array):
        return lax.ppermute(array, "tensor", [(t, t ^ 1) for t in range(2 * NX)])

    def spread(array):
        return [array] + [shift(array, -s) for s in (1, 2, 3)]

    def collect(parts):
        return [parts[0]] + [shift(parts[s], s) for s in (1, 2, 3)]

    tie = lax.optimization_barrier

    seen = []

    def attention(layer, message, beside, *late, ahead=()):
        arrived = lax.all_to_all(message, "tm", 0, 0, tiled=True)
        arrived, *late = tie((arrived, *late))
        arrived_par = swap(arrived)
        seen.append(beside())
        if layer == 1:
            late = [seen[1]]
        order, mask, row_time = seen[0]
        arrived, arrived_par, *late = tie((arrived, arrived_par, *late))
        late = [swap(a) for a in late]
        mixed = call(
            functools.partial(attn_kernel, layer),
            (order, mask, row_time, arrived, arrived_par),
            jax.ShapeDtypeStruct((PARTS, 24, 128), jnp.bfloat16),
            [
                pltpu.VMEM((256, KEYS), jnp.bfloat16),
                pltpu.VMEM((KEYS, 128), jnp.bfloat16),
                pltpu.VMEM((3, 256, KEYS), jnp.float32),
                pltpu.VMEM((3, 256, KEYS), jnp.bfloat16),
            ],
            scalars=1,
            limit=24,
        )
        mixed, *late = tie((mixed, *late, *ahead))
        back = lax.all_to_all(mixed, "tm", 0, 0, tiled=True)
        return tie((back, *late))

    message_shape = jax.ShapeDtypeStruct((PARTS, 56, 128), jnp.bfloat16)

    def in_hbm(*arrays):
        return [pltpu.with_memory_space_constraint(a, pltpu.HBM) for a in arrays]

    biases = jnp.transpose(qkv_bias, (1, 0, 2))
    held, wide, raw, w_own = call(
        pack_kernel,
        in_hbm(qkv_weight, out_weight, biases, frames_in),
        [
            jax.ShapeDtypeStruct((4, HELD, 128), jnp.bfloat16),
            jax.ShapeDtypeStruct((D, 128), jnp.bfloat16),
            block(rows=8 * BLOCK),
            jax.ShapeDtypeStruct((3, D, 128), jnp.bfloat16),
        ],
        [pltpu.VMEM((3, LAYERS, 128), jnp.float32), pltpu.SemaphoreType.DMA((20,))],
        in_specs=[HBM] * 4,
    )
    held, late_qkv, late_biases, late_fc2 = tie((held, qkv_weight, biases, fc2_weight))
    qkv_par = swap(late_qkv)
    biases_par = swap(late_biases)
    fc2_par = swap(late_fc2)
    helds = spread(held)
    held_par = swap(held)
    xrows, message = call(
        start_kernel,
        (raw, w_own, qkv_par, biases, biases_par, ln1_gain, ln1_bias),
        [block(rows=NX * PAD), message_shape],
        [pltpu.VMEM((8 * BLOCK, D), jnp.float32), pltpu.VMEM((NX * PAD, D), jnp.bfloat16)],
    )
    message = tie(message)

    def tables():
        return call(
            tables_kernel,
            (frame_time, cond_count),
            [
                jax.ShapeDtypeStruct((FRAMES,), jnp.int32),
                jax.ShapeDtypeStruct((FRAMES, KEYS), jnp.bfloat16),
                jax.ShapeDtypeStruct((PARTS, 128), jnp.int32),
            ],
            scalars=2,
            out_specs=[SMEM, VMEM, VMEM],
        )

    back, fc1_par, fc1_bias_par, fc2_par, held_par = attention(
        0, message, tables, fc1_weight, fc1_bias, ahead=(fc2_par, held_par)
    )
    heads = call(heads_kernel, (back,), jax.ShapeDtypeStruct((NX * PAD, 256), jnp.bfloat16))
    loaded = call(plane_kernel, helds, jax.ShapeDtypeStruct((NX, D, 128), jnp.bfloat16))
    loaded_par = swap(loaded)
    heads, wide = tie((heads, wide))
    heads = spread(heads)
    wides = spread(wide)
    packed_a, packed_b, w1, w2 = call(
        load_mlp_kernel,
        in_hbm(fc1_weight, fc1_bias, fc2_weight),
        [
            jax.ShapeDtypeStruct((2, HELD, 256), jnp.bfloat16),
            jax.ShapeDtypeStruct((2, HELD, 256), jnp.bfloat16),
            jax.ShapeDtypeStruct((D, 512), jnp.bfloat16),
            jax.ShapeDtypeStruct((512, D), jnp.bfloat16),
        ],
        [pltpu.VMEM((LAYERS, 512), jnp.float32), pltpu.SemaphoreType.DMA((13,))],
        in_specs=[HBM] * 3,
    )
    held_pars = [held_par] + [swap(helds[s]) for s in (1, 2, 3)]
    everything = (*helds, *held_pars)
    first, normed_two = call(
        every_out_kernel,
        (*heads, xrows, out_bias, ln2_gain, ln2_bias, loaded, loaded_par),
        [block(jnp.float32), block(rows=NX * PAD)],
        [pltpu.VMEM((NX * PAD, D), jnp.bfloat16)],
        scalars=0,
    )
    partial = {}
    for group in GROUPS:
        done = call(
            functools.partial(mlp_kernel, group),
            (normed_two, w1, fc1_par, fc1_bias, fc1_bias_par, w2, fc2_par),
            [block()] * len(group),
            [pltpu.VMEM((PAD * len(group), D), jnp.bfloat16)],
            scalars=0,
        )
        partial.update(zip(group, done))

    def pair(array, other):
        return lax.ppermute(array, "tensor", [(t, other(t // 2) * 2 + t % 2) for t in range(2 * NX)])

    far_a = pair(packed_a, lambda c: c ^ 1)
    far_b = pair(packed_b, lambda c: c ^ 1)
    partial = collect(partial)
    stream, message = call(
        turn_kernel,
        (first, *partial, fc2_bias, ln1_gain, ln1_bias, *everything),
        [block(), message_shape],
        [pltpu.VMEM((PAD, D), jnp.bfloat16), pltpu.VMEM((2 * NX, 3, PAD, 128), jnp.float32)],
    )

    def stack():
        return call(stack_kernel, wides, jax.ShapeDtypeStruct((NX, D, 128), jnp.bfloat16))

    back, out_par = attention(1, message, stack)
    first, normed_two = call(
        whole_out_kernel,
        (back, stream, out_bias, ln2_gain, ln2_bias, seen[1], out_par),
        [block(jnp.float32), block()],
        [pltpu.VMEM((PAD, D), jnp.bfloat16)],
    )
    moved = pair(normed_two, lambda c: 3 - c)
    pad = [pltpu.VMEM((PAD, D), jnp.bfloat16)]
    shared = (fc1_par, fc1_bias_par, fc2_par, packed_a, packed_b, far_a)
    far_a_par = swap(far_a)
    total = call(own_mlp_kernel, (first, normed_two, fc2_bias, *shared), block(jnp.float32), pad)
    total, last_half = tie((total, far_b))
    far_b_par = swap(last_half)
    total = call(half_mlp_kernel, (total, normed_two, far_b, far_a_par), block(jnp.float32), pad)
    passed = call(
        moved_mlp_kernel, (moved, *shared, far_a_par, far_b), block(jnp.float32, PAD), pad
    )
    keep, send, here, there = call(
        end_mlp_kernel,
        (total, passed, normed_two, moved, far_b_par),
        [block(jnp.float32), block(jnp.float32, 32), block(rows=40), block(rows=32)],
        [pltpu.VMEM((2 * PAD, D), jnp.bfloat16)],
    )
    here = pair(here, lambda c: 3 - c)
    other = swap(send)
    cross = [(t, (3 - t // 2) * 2 + 1 - t % 2) for t in range(2 * NX)]
    there = lax.ppermute(there, "tensor", cross)
    return call(
        last_kernel, (keep, other, here, there), jax.ShapeDtypeStruct((1, BLOCK, D), jnp.bfloat16)
    )


def solution(mesh):
    in_specs = (
        P("tm", None, None),
        P(),
        P(),
        P(),
        P(),
        P(None, None, None, "tensor"),
        P(None, None, "tensor"),
        P(None, "tensor", None),
        P(),
        P(),
        P(),
        P(None, None, "tensor"),
        P(None, "tensor"),
        P(None, "tensor", None),
        P(),
    )
    out_specs = P("tm", "tensor", None)
    return jax.shard_map(shards, mesh=mesh, in_specs=in_specs, out_specs=out_specs, check_vma=False)
```
